32 devices in a mesh: grp: 2 (over y), seq: 16 (over z, x, core), head: 1.
Axes of the slice: x: 2, y: 2, z: 4, core: 2. Of those that a mesh axis runs over, the one named last changes fastest.
Arguments:
- queries: bfloat16 [2048, 1, 128], P(('grp', 'seq'), 'head'), parts along dimension 0, may hold values from -6 to 6
- keys: bfloat16 [256, 512, 8, 128], P(('grp', 'seq'), None, 'head'), parts along dimension 0, may hold values from -28 to 28
- values: bfloat16 [256, 512, 8, 128], P(('grp', 'seq'), None, 'head'), parts along dimension 0, may hold values from -6 to 6
- lengths: int32 [32], P('grp'), parts along dimension 0, may hold values from 1 to 4096, 40960 in all
- slot_block: int32 [256], P(('grp', 'seq')), parts along dimension 0, may hold values from 0 to 127, each once
Outputs:
- attended: bfloat16 [2048, 1, 128], P(('grp', 'seq'), 'head'), parts along dimension 0
The draws below stay inside these ranges and needn't reach their ends.
There are 2 independent parts, one for each index of `grp`. The reference program is written for one: setup_inputs(seed, part) draws one part's arguments, and reference() takes and returns one part's arrays. A program takes and returns all parts, laid end to end along the dimension named above; each array names one. Nothing has to cross between parts.
Inputs may be any that keep to these rules, and one draw needn't show every extreme that they name: `slot_block`: each slot holds a different logical block; every block of every sequence has a slot. `lengths`: every sequence has at least one token.
All inputs are finite; a program needn't handle non-finite values.
Results may differ from the reference program's by a relative error of at most 0.0055.
Values may be sent and summed in bfloat16 or wider, within the bound.
A program may use at most 64 MiB of HBM per device.

```python
import math
import jax
import jax.numpy as jnp
import numpy as np
from jax import lax

QH = 64
KVH = 8
HD = 128
BLK = 512
BATCH = 16
SLOTS = 128
MAXLEN = 4096
N_HEAD = 1


def draw_queries(key, part):
    base = jnp.clip(jax.random.normal(jax.random.fold_in(key, 21), (BATCH, QH, HD), jnp.float32), -6.0, 6.0)
    base = base.reshape(BATCH, N_HEAD, QH // N_HEAD, HD).transpose(0, 2, 1, 3)
    return base.reshape(BATCH * QH // N_HEAD, N_HEAD, HD).astype(jnp.bfloat16)


def draw_keys(key, part):
    base = jnp.clip(3.0 * jax.random.normal(jax.random.fold_in(key, 31), (SLOTS, BLK, KVH, HD), jnp.float32), -18.0, 18.0)
    return base.astype(jnp.bfloat16)


def steps_of(rng, shape, pieces, low, top_value):
    factor_of = 1.0
    for axis_at, shards_of in pieces:
        draws = jax.random.uniform(jax.random.fold_in(jax.random.fold_in(rng, 6), axis_at), (shards_of,), jnp.float32, low / len(pieces), top_value / len(pieces))
        factor_of = factor_of * jnp.repeat(jnp.exp(draws), shape[axis_at] // shards_of).reshape((-1,) + (1,) * (len(shape) - 1 - axis_at))
    return factor_of


def length_profile(number_of, total, most, lean):
    portions = [(1 << 20) // math.isqrt(rank ** lean) + 1 for rank in range(2, number_of + 1)]
    surplus, counts = total - most - (number_of - 1), [1] * (number_of - 1)
    while surplus > 0:
        candidates = [i for i in range(number_of - 1) if counts[i] < most]
        mass, remaining = sum([portions[i] for i in candidates]), surplus
        for i in candidates:
            more = min(most - counts[i], max(1, remaining * portions[i] // mass), surplus)
            counts[i] = counts[i] + more
            surplus = surplus - more
    return np.array([most] + counts)


def ragged_sizes(key, number_of, total, limit, lean):
    if number_of == 2:
        one = jax.random.randint(key, (), max(1, total - limit), min(limit, total - 1) + 1)
        return jnp.stack([one, total - one])
    sizes = jnp.asarray(length_profile(number_of, total, limit, lean), jnp.int32)
    couples = (number_of - 1) // 2
    giver, taker = sizes[1:1 + 2 * couples:2], sizes[2:2 + 2 * couples:2]
    margin = jnp.minimum(giver - 1, limit - taker)
    passed = jax.random.randint(jax.random.fold_in(key, 1), (couples,), 0, 1 << 20) % (margin + 1)
    sizes = sizes.at[1:1 + 2 * couples:2].set(giver - passed).at[2:2 + 2 * couples:2].set(taker + passed)
    return sizes[jax.random.permutation(jax.random.fold_in(key, 2), number_of)]


def bell_draw(stream_key, extent, width, reach, split=(), held_as=jnp.bfloat16):
    values = jax.random.normal(stream_key, extent, jnp.float32) * width
    if len(split) > 0:
        values = steps_of(stream_key, extent, split, -0.22, 0.18) * values
    return jnp.clip(values, min=-reach, max=reach).astype(held_as)


def setup_inputs(seed: int = 0, part: int = 0) -> dict:
    seeds = jax.random.split(jax.random.key(seed), 6)
    part_splits = jax.random.split(jax.random.fold_in(seeds[5], part), 6)
    queries = draw_queries(jax.random.fold_in(jax.random.fold_in(seeds[5], part), 71), part)
    keys = draw_keys(jax.random.fold_in(jax.random.fold_in(seeds[5], part), 71), part)
    values = bell_draw(part_splits[2], (SLOTS, BLK, KVH, HD), 1.0, 6.0, ((0, 16),))
    lengths = ragged_sizes(part_splits[3], BATCH, 5 * MAXLEN // 8 * BATCH, MAXLEN, 1).astype(jnp.int32)
    slot_block = jax.random.permutation(part_splits[4], SLOTS).astype(jnp.int32)
    return {"queries": queries, "keys": keys, "values": values, "lengths": lengths, "slot_block": slot_block}


def reference(queries, keys, values, lengths, slot_block):
    per_half = QH // N_HEAD
    group = QH // KVH
    per_seq = SLOTS // BATCH
    factor = HD ** -0.5
    q_full = queries.reshape(BATCH, per_half, N_HEAD, HD).transpose(0, 2, 1, 3).reshape(BATCH, KVH, group, HD)

    def one_slot(packed):
        key_blk, val_blk, code = packed
        seq_id = (code // per_seq).astype(jnp.int32)
        blk_id = (code % per_seq).astype(jnp.int32)
        q_one = lax.dynamic_index_in_dim(q_full, seq_id, 0, keepdims=False)
        scores = jnp.einsum('kgd,tkd->kgt', q_one.astype(jnp.float32), key_blk.astype(jnp.float32), precision=lax.Precision.HIGHEST) * factor
        positions = blk_id * BLK + jnp.arange(BLK, dtype=jnp.int32)
        live = (positions < lengths[seq_id])[None, None, :]
        peak = jnp.max(jnp.where(live, scores, -1e30), axis=-1)
        weights = jnp.where(live, jnp.exp(scores - peak[..., None]), 0.0).astype(jnp.bfloat16)
        total = jnp.sum(weights.astype(jnp.float32), axis=-1)
        partial_out = jnp.einsum('kgt,tkd->kgd', weights.astype(jnp.float32), val_blk.astype(jnp.float32), precision=lax.Precision.HIGHEST)
        return peak, total, partial_out

    peaks, totals, partials = lax.map(one_slot, (keys, values, slot_block))
    seq_of = (slot_block // per_seq).astype(jnp.int32)
    member = seq_of[:, None] == jnp.arange(BATCH, dtype=jnp.int32)[None, :]
    best = jnp.max(jnp.where(member[:, :, None, None], peaks[:, None], -1e30), axis=0)
    scaled = jnp.exp(peaks - jnp.take(best, seq_of, axis=0))
    denom = jax.ops.segment_sum(scaled * totals, seq_of, BATCH)
    numer = jax.ops.segment_sum(scaled[..., None] * partials, seq_of, BATCH)
    result = numer / denom[..., None]
    result = result.reshape(BATCH, N_HEAD, per_half, HD).transpose(0, 2, 1, 3).reshape(BATCH * per_half, N_HEAD, HD)
    return result.astype(jnp.bfloat16)
```

```python
import functools
import math
import jax
import jax.numpy as jnp
from jax import lax
from jax.experimental import pallas as pl
from jax.experimental.pallas import tpu as pltpu
from jax.sharding import PartitionSpec as P

LANES = 128
MESH_ID = pl.DeviceIdType.MESH
LOW = -1e30
DEAD = -3e38
PAIR = 2


def fold(tile, step, op):
    shift = LANES // 2
    while shift >= step:
        tile = op(tile, pltpu.roll(tile, shift, 1))
        shift //= 2
    return tile


def kernel(
    n, batch, block, kv, factor,
    lengths_hbm, block_hbm, q_hbm, k_hbm, v_hbm, out_ref,
    lengths, slot_block, q_ref, q_all, k_buf, v_buf, base, scores, parts, peaks, totals,
    best_own, best_in, joint, tot_own, tot_in, acc, acc_send, acc_in, stat, acc2, stat2, acc2_in, stat2_in,
    k_sem, v_sem, own_sem, in_sem, qs_sem, qr_sem, fs_sem, bs_sem, br_sem, ps_sem, pr_sem, ts_sem, tr_sem,
    as_sem, ar_sem, ss_sem, sr_sem,
):
    slots = k_buf.shape[0]
    hd = q_ref.shape[1]
    share = q_ref.shape[0]
    outer = n // 2
    per = n // batch
    blocks = slots * n // batch
    heads = per * share
    group = heads // kv
    duo = PAIR * group
    span = PAIR * duo
    groups = heads // span
    rows = share // groups
    quarters = LANES // span
    rep = block * PAIR // quarters
    me = lax.axis_index("seq")
    mine, inner = me // 2, me % 2
    partner = me + 1 - 2 * inner
    k_rows = k_buf.reshape(slots, kv // PAIR, block * PAIR, hd)
    v_rows = v_buf.reshape(slots, kv // PAIR, block * PAIR, hd)

    def k_copy(s, p):
        return pltpu.make_async_copy(k_hbm.at[s, :, p], k_buf.at[s, p], k_sem.at[s, p])

    def v_copy(s, p):
        return pltpu.make_async_copy(v_hbm.at[s, :, p], v_buf.at[s, p], v_sem.at[s, p])

    def remote(src, dst, ssem, rsem, dev):
        return pltpu.make_async_remote_copy(
            src_ref=src, dst_ref=dst, send_sem=ssem, recv_sem=rsem,
            device_id={"seq": dev}, device_id_type=MESH_ID,
        )

    q_in = pltpu.make_async_copy(q_hbm, q_ref, in_sem.at[0])
    q_in.start()
    peers = [(mine + r) % outer for r in range(1, outer)]
    barrier = pltpu.get_barrier_semaphore()
    for o in peers:
        pl.semaphore_signal(barrier, inc=1, device_id={"seq": o * 2 + inner}, device_id_type=MESH_ID)
    pl.semaphore_signal(barrier, inc=1, device_id={"seq": partner}, device_id_type=MESH_ID)
    len_in = pltpu.make_async_copy(lengths_hbm, lengths, in_sem.at[1])
    block_in = pltpu.make_async_copy(block_hbm, slot_block, in_sem.at[2])
    len_in.start()
    block_in.start()
    own = pltpu.make_async_copy(q_hbm, q_all.at[me], own_sem)
    own.start()
    for g in range(groups):
        for s in range(slots):
            for p in range(PAIR):
                k_copy(s, PAIR * g + p).start()
    for g in range(groups):
        for s in range(slots):
            for p in range(PAIR):
                v_copy(s, PAIR * g + p).start()

    row = lax.broadcasted_iota(jnp.int32, (rep, LANES), 0)
    col = lax.broadcasted_iota(jnp.int32, (rep, LANES), 1)
    base[...] = jnp.where(row % PAIR == col // group % PAIR, row, 1 << 24) + col // span * rep
    q_in.wait()
    pl.semaphore_wait(barrier, outer)

    sends = []
    for r, o in enumerate(peers):
        sends.append(remote(q_ref, q_all.at[me], qs_sem.at[r], qr_sem.at[me], o * 2 + inner))
    sends.append(remote(q_ref, q_all.at[me], qs_sem.at[outer - 1], qr_sem.at[me], partner))
    for c in sends:
        c.start()
    for r in range(1, outer):
        src = ((mine + outer - r) % outer) * 2 + inner
        remote(q_ref, q_all.at[src], qs_sem.at[0], qr_sem.at[src], partner).wait_recv()
        c = remote(q_all.at[src], q_all.at[src], fs_sem.at[r - 1], qr_sem.at[src], partner)
        c.start()
        sends.append(c)
    len_in.wait()
    block_in.wait()
    own.wait()
    remote(q_ref, q_all.at[partner], qs_sem.at[0], qr_sem.at[partner], partner).wait_recv()
    for r in range(1, outer):
        src = ((mine + outer - r) % outer) * 2 + 1 - inner
        remote(q_ref, q_all.at[src], qs_sem.at[0], qr_sem.at[src], partner).wait_recv()

    lane = lax.broadcasted_iota(jnp.int32, (batch, LANES), 1)
    which = lax.broadcasted_iota(jnp.int32, (batch, LANES), 0)
    seqs = [slot_block[s] // blocks for s in range(slots)]

    def score(g, s):
        code = slot_block[s]
        seq, blk = code // blocks, code % blocks
        limit = (lengths[seq] - blk * block) * PAIR
        if per > 1:
            q = q_all[pl.ds(seq * per, per)].astype(jnp.float32).reshape(heads, hd).astype(jnp.bfloat16)
        else:
            q = q_all[seq, g * span : (g + 1) * span]
        blank = jnp.zeros((duo, hd), jnp.bfloat16)
        pair = jnp.concatenate(
            [jnp.concatenate([q[:duo], blank], axis=0), jnp.concatenate([blank, q[duo:]], axis=0)], axis=1
        )
        total = jnp.zeros((rep, LANES), jnp.float32)
        for u in range(quarters):
            at = pl.ds(u * rep, rep)
            keys = jnp.concatenate([k_rows[s, PAIR * g, at, :], k_rows[s, PAIR * g + 1, at, :]], axis=1)
            place = [pair if w == u else jnp.zeros_like(pair) for w in range(quarters)]
            total = total + lax.dot_general(
                keys, jnp.concatenate(place, axis=0), (((1,), (1,)), ((), ())),
                preferred_element_type=jnp.float32,
            )
        masked = jnp.where(base[...] < limit, total * factor, DEAD)
        scores[g, s] = masked
        top = jnp.maximum(jnp.max(masked, axis=0, keepdims=True), LOW)
        peaks[g, pl.ds(s, 1), :] = fold(top, span, jnp.maximum)

    def weigh(g, s):
        seq = slot_block[s] // blocks
        weight = jnp.exp2(scores[g, s] - joint[g, pl.ds(seq, 1), :]).astype(jnp.bfloat16)
        total = jnp.sum(weight.astype(jnp.float32), axis=0, keepdims=True)
        totals[g, pl.ds(s, 1), :] = fold(total, span, jnp.add)
        turned = weight.T
        out = jnp.zeros((span, PAIR * hd), jnp.float32)
        for u in range(quarters):
            at = pl.ds(u * rep, rep)
            vals = jnp.concatenate([v_rows[s, PAIR * g, at, :], v_rows[s, PAIR * g + 1, at, :]], axis=1)
            out = out + jnp.dot(
                turned[u * span : (u + 1) * span], vals, preferred_element_type=jnp.float32
            )
        parts[s] = jnp.concatenate([out[:duo, :hd], out[duo:, hd:]], axis=0)

    def loop(step):
        def one(s, carry):
            step(s)
            return carry
        lax.fori_loop(0, slots, one, 0, unroll=4)

    swaps = []
    for g in range(groups):
        for s in range(slots):
            for p in range(PAIR):
                k_copy(s, PAIR * g + p).wait()
        loop(functools.partial(score, g))
        best = jnp.full((batch, LANES), LOW, jnp.float32)
        for s in range(slots):
            best = jnp.maximum(best, jnp.where(which == seqs[s], peaks[g, s : s + 1, :], LOW))
        best_own[g] = best
        c = remote(best_own.at[g], best_in.at[g], bs_sem.at[g], br_sem.at[g], partner)
        c.start()
        swaps.append(c)

    def spread_out(g):
        total = jnp.zeros((batch, LANES), jnp.float32)
        for s in range(slots):
            total = total + jnp.where(which == seqs[s], totals[g, s : s + 1, :], 0.0)
        tot_own[g] = total
        for b in range(batch):
            out = jnp.zeros((span, hd), jnp.float32)
            for s in range(slots):
                out = out + jnp.where(seqs[s] == b, 1.0, 0.0) * parts[s]
            for p in range(per):
                j = b * per + p
                piece = out[p * rows : (p + 1) * rows]
                acc[g, j % 2, j // 2] = piece
                acc_send[g, j % 2, j // 2] = piece.astype(jnp.bfloat16)
        c1 = remote(acc_send.at[g, 1 - inner], acc_in.at[g], ps_sem.at[g], pr_sem.at[g], partner)
        c2 = remote(tot_own.at[g], tot_in.at[g], ts_sem.at[g], tr_sem.at[g], partner)
        c2.start()
        c1.start()
        return [c1, c2]

    def exchange(g):
        total = tot_own[g] + tot_in[g]
        both = jnp.where(lane % (PAIR * span) < span, joint[g], total)
        for j in range(n):
            b, p = j // per, j % per
            line = both[b : b + 1]
            if p:
                line = pltpu.roll(line, LANES - p * rows, 1)
            stat[g, j % 2, j // 2] = line
        made = []
        for r in range(1, outer + 1):
            o = (mine + r) % outer
            whole = (acc[g, inner, o] + acc_in[g, o].astype(jnp.float32)).astype(jnp.bfloat16)
            if r == outer:
                acc2_in[g, o] = whole
                stat2_in[g, o] = stat[g, inner, o]
                break
            acc2[g, o] = whole
            stat2[g, o] = stat[g, inner, o]
            dev = o * 2 + inner
            c1 = remote(acc2.at[g, o], acc2_in.at[g, mine], as_sem.at[g, r - 1], ar_sem.at[g, mine], dev)
            c2 = remote(stat2.at[g, o], stat2_in.at[g, mine], ss_sem.at[g, r - 1], sr_sem.at[g, mine], dev)
            c2.start()
            c1.start()
            made += [c1, c2]
        return made

    last = []
    for g in range(groups):
        swaps[g].wait()
        joint[g] = jnp.maximum(best_own[g], best_in[g])
        for s in range(slots):
            for p in range(PAIR):
                v_copy(s, PAIR * g + p).wait()
        loop(functools.partial(weigh, g))
        gone = spread_out(g)
        for c in gone:
            c.wait()
        last += exchange(g)

    for g in range(groups):
        for r in range(1, outer):
            o = (mine + outer - r) % outer
            remote(stat2.at[g, o], stat2_in.at[g, o], ss_sem.at[g, 0], sr_sem.at[g, o], partner).wait_recv()
            remote(acc2.at[g, o], acc2_in.at[g, o], as_sem.at[g, 0], ar_sem.at[g, o], partner).wait_recv()
        tops = stat2_in[g].reshape(outer, LANES)
        best = jnp.max(tops, axis=0, keepdims=True)
        scale = jnp.exp2(tops - best)
        total = pltpu.roll(tops, LANES - span, 1)
        scale = scale / jnp.sum(scale * total, axis=0, keepdims=True)
        turned = scale.T
        out = jnp.zeros((rows, hd), jnp.float32)
        for o in range(outer):
            out = out + turned[:rows, o : o + 1] * acc2_in[g, o].astype(jnp.float32)
        out_ref[g * rows : (g + 1) * rows] = out.astype(jnp.bfloat16)
    for c in sends + last:
        c.wait_send()


def body(queries, keys, values, lengths, slot_block):
    slots, block, kv, hd = keys.shape
    share = queries.shape[0]
    n = lax.axis_size("seq")
    batch = lengths.shape[0]
    per = n // batch
    heads = per * share
    duo = PAIR * heads // kv
    span = PAIR * duo
    groups = heads // span
    rows = share // groups
    outer = n // 2
    rep = block * PAIR * span // LANES
    pairs = kv // PAIR
    assert groups == 1 or per == 1
    f32, bf16 = jnp.float32, jnp.bfloat16
    dma = pltpu.SemaphoreType.DMA
    vmem = pl.BlockSpec(memory_space=pltpu.VMEM)
    hbm = pl.BlockSpec(memory_space=pltpu.HBM)
    result = pl.pallas_call(
        functools.partial(kernel, n, batch, block, kv, hd ** (-0.5) * math.log2(math.e)),
        out_shape=jax.ShapeDtypeStruct((share, hd), bf16),
        in_specs=[hbm] * 5,
        out_specs=vmem,
        scratch_shapes=[
            pltpu.SMEM(lengths.shape, jnp.int32),
            pltpu.SMEM(slot_block.shape, jnp.int32),
            pltpu.VMEM((share, hd), bf16),
            pltpu.VMEM((n, share, hd), bf16),
            pltpu.VMEM((slots, pairs, block, PAIR, hd), bf16),
            pltpu.VMEM((slots, pairs, block, PAIR, hd), bf16),
            pltpu.VMEM((rep, LANES), jnp.int32),
            pltpu.VMEM((groups, slots, rep, LANES), f32),
            pltpu.VMEM((slots, span, hd), f32),
            pltpu.VMEM((groups, slots, LANES), f32),
            pltpu.VMEM((groups, slots, LANES), f32),
            pltpu.VMEM((groups, batch, LANES), f32),
            pltpu.VMEM((groups, batch, LANES), f32),
            pltpu.VMEM((groups, batch, LANES), f32),
            pltpu.VMEM((groups, batch, LANES), f32),
            pltpu.VMEM((groups, batch, LANES), f32),
            pltpu.VMEM((groups, 2, outer, rows, hd), f32),
            pltpu.VMEM((groups, 2, outer, rows, hd), bf16),
            pltpu.VMEM((groups, outer, rows, hd), bf16),
            pltpu.VMEM((groups, 2, outer, 1, LANES), f32),
            pltpu.VMEM((groups, outer, rows, hd), bf16),
            pltpu.VMEM((groups, outer, 1, LANES), f32),
            pltpu.VMEM((groups, outer, rows, hd), bf16),
            pltpu.VMEM((groups, outer, 1, LANES), f32),
            dma((slots, pairs)), dma((slots, pairs)), dma, dma((3,)),
            dma((outer,)), dma((n,)), dma((outer,)),
            dma((groups,)), dma((groups,)), dma((groups,)), dma((groups,)), dma((groups,)), dma((groups,)),
            dma((groups, outer)), dma((groups, outer)), dma((groups, outer)), dma((groups, outer)),
        ],
        compiler_params=pltpu.CompilerParams(
            collective_id=0, has_side_effects=True, vmem_limit_bytes=67043328
        ),
        name="decode",
    )(
        lengths,
        slot_block,
        queries.reshape(share, hd),
        keys.reshape(slots, block, pairs, PAIR, hd),
        values.reshape(slots, block, pairs, PAIR, hd),
    )
    return result.reshape(share, 1, hd)


def solution(mesh):
    placed = (
        P(("grp", "seq"), "head", None),
        P(("grp", "seq"), None, "head", None),
        P(("grp", "seq"), None, "head", None),
        P("grp"),
        P(("grp", "seq")),
    )
    return jax.shard_map(
        body, mesh=mesh, in_specs=placed, out_specs=P(("grp", "seq"), "head", None), check_vma=False
    )
```

```python
import functools
import math
import jax
import jax.numpy as jnp
from jax import lax
from jax.experimental import pallas as pl
from jax.experimental.pallas import tpu as pltpu
from jax.sharding import PartitionSpec as P

LANES = 128
MESH_ID = pl.DeviceIdType.MESH
LOW = -1e30
DEAD = -3e38


def fold(tile, step, op):
    shift = LANES // 2
    while shift >= step:
        tile = op(tile, pltpu.roll(tile, shift, 1))
        shift //= 2
    return tile


def spread(tile, start, heads):
    group = tile.shape[0]
    return jnp.concatenate(
        [jnp.broadcast_to(tile[:, start + h : start + h + 1], (group, LANES)) for h in range(heads)],
        axis=0,
    )


def unpack(tile, lane):
    turned = pltpu.roll(tile, LANES // 2, 1)
    low = lane < LANES // 2
    return jnp.where(low, tile, turned), jnp.where(low, turned, tile)


def kernel(
    n, batch, block, kv, factor,
    lengths_hbm, block_hbm, q_hbm, k_hbm, v_hbm, out_ref,
    lengths, slot_block, final, q_ref, q_all, k_buf, v_buf, scores, sums, peaks, totals,
    best_own, best_in, tot_own, tot_in, acc_send, acc_in, acc2, stat2, acc2_in, stat2_in,
    k_sem, v_sem, own_sem, in_sem, qs_sem, qr_sem, fs_sem, swap_sem, as_sem, ar_sem, ss_sem, sr_sem,
):
    slots, cols, hd = k_buf.shape
    share = q_ref.shape[0]
    outer = n // 2
    per = n // batch
    blocks = slots * n // batch
    heads = per * share
    group = heads // kv
    held = share // group
    half = cols // 2
    me = lax.axis_index("seq")
    mine, inner = me // 2, me % 2
    partner = me + 1 - 2 * inner

    def k_copy(s):
        return pltpu.make_async_copy(k_hbm.at[s], k_buf.at[s], k_sem.at[s])

    def v_copy(s):
        return pltpu.make_async_copy(v_hbm.at[s], v_buf.at[s], v_sem.at[s])

    def remote(src, dst, ssem, rsem, dev):
        return pltpu.make_async_remote_copy(
            src_ref=src, dst_ref=dst, send_sem=ssem, recv_sem=rsem,
            device_id={"seq": dev}, device_id_type=MESH_ID,
        )

    q_in = pltpu.make_async_copy(q_hbm, q_ref, in_sem.at[0])
    q_in.start()
    peers = [(mine + r) % outer for r in range(1, outer)]
    barrier = pltpu.get_barrier_semaphore()
    for o in peers:
        pl.semaphore_signal(barrier, inc=1, device_id={"seq": o * 2 + inner}, device_id_type=MESH_ID)
    pl.semaphore_signal(barrier, inc=1, device_id={"seq": partner}, device_id_type=MESH_ID)
    len_in = pltpu.make_async_copy(lengths_hbm, lengths, in_sem.at[1])
    block_in = pltpu.make_async_copy(block_hbm, slot_block, in_sem.at[2])
    len_in.start()
    block_in.start()
    own = pltpu.make_async_copy(q_hbm, q_all.at[me], own_sem)
    own.start()
    for s in range(slots):
        k_copy(s).start()
    for s in range(slots):
        v_copy(s).start()
    sums[...] = jnp.zeros_like(sums)
    len_in.wait()
    block_in.wait()
    seqs = [slot_block[s] // blocks for s in range(slots)]
    before = []
    for s in range(slots):
        prev = slots
        for t in range(s):
            prev = jnp.where(seqs[t] == seqs[s], t, prev)
        before.append(prev)
    for b in range(batch):
        last = slots
        for s in range(slots):
            last = jnp.where(seqs[s] == b, s, last)
        final[b] = last
    q_in.wait()
    pl.semaphore_wait(barrier, outer)

    sends = []
    for r, o in enumerate(peers):
        sends.append(remote(q_ref, q_all.at[me], qs_sem.at[r], qr_sem.at[me], o * 2 + inner))
    sends.append(remote(q_ref, q_all.at[me], qs_sem.at[outer - 1], qr_sem.at[me], partner))
    for c in sends:
        c.start()
    for r in range(1, outer):
        src = ((mine + outer - r) % outer) * 2 + inner
        remote(q_ref, q_all.at[src], qs_sem.at[0], qr_sem.at[src], partner).wait_recv()
        c = remote(q_all.at[src], q_all.at[src], fs_sem.at[r - 1], qr_sem.at[src], partner)
        c.start()
        sends.append(c)
    own.wait()
    remote(q_ref, q_all.at[partner], qs_sem.at[0], qr_sem.at[partner], partner).wait_recv()
    for r in range(1, outer):
        src = ((mine + outer - r) % outer) * 2 + 1 - inner
        remote(q_ref, q_all.at[src], qs_sem.at[0], qr_sem.at[src], partner).wait_recv()

    lane = lax.broadcasted_iota(jnp.int32, (group, LANES), 1)
    home = lane // kv
    chunk = min(half, 512)
    wide = lax.broadcasted_iota(jnp.int32, (group, chunk), 1)
    picks = [wide % kv == h for h in range(kv)]

    def score(s):
        code = slot_block[s]
        seq, blk = code // blocks, code % blocks
        limit = (lengths[seq] - blk * block) * kv
        q = q_all[pl.ds(seq * per, per)]
        if per > 1:
            q = q.astype(jnp.float32).reshape(heads, hd).astype(jnp.bfloat16)
        else:
            q = q.reshape(heads, hd)
        blank = jnp.zeros_like(q)
        both = jnp.concatenate(
            [jnp.concatenate([q, blank], axis=0), jnp.concatenate([blank, q], axis=0)], axis=1
        )
        top = jnp.full((group, LANES), LOW, jnp.float32)
        for c in range(0, half, chunk):
            keys = jnp.concatenate(
                [k_buf[s, c : c + chunk, :], k_buf[s, half + c : half + c + chunk, :]], axis=1
            )
            full = lax.dot_general(
                both, keys, (((1,), (1,)), ((), ())), preferred_element_type=jnp.float32
            )
            for x, at in ((0, c), (heads, half + c)):
                packed = full[x : x + group]
                for h in range(1, kv):
                    packed = jnp.where(picks[h], full[x + h * group : x + (h + 1) * group], packed)
                packed = jnp.where(wide < limit - at, packed * factor, DEAD)
                scores[s, :, at : at + chunk] = packed
                for l in range(0, chunk, LANES):
                    top = jnp.maximum(top, packed[:, l : l + LANES])
        peaks[s] = fold(top, kv, jnp.maximum)

    def weigh(s):
        top = jnp.concatenate([peaks[s]] * (chunk // LANES), axis=1)
        total = jnp.zeros((group, LANES), jnp.float32)
        out = jnp.zeros((2 * heads, 2 * hd), jnp.float32)
        for c in range(0, half, chunk):
            rows = []
            for at in (c, half + c):
                weight = jnp.exp2(scores[s, :, at : at + chunk] - top).astype(jnp.bfloat16)
                weight = weight.astype(jnp.float32)
                for l in range(0, chunk, LANES):
                    total = total + weight[:, l : l + LANES]
                rows += [jnp.where(picks[h], weight, 0.0) for h in range(kv)]
            vals = jnp.concatenate(
                [v_buf[s, c : c + chunk, :], v_buf[s, half + c : half + c + chunk, :]], axis=1
            )
            out = out + jnp.dot(
                jnp.concatenate(rows, axis=0).astype(jnp.bfloat16), vals,
                preferred_element_type=jnp.float32,
            )
        sums[s] = out[:heads, :hd] + out[heads:, hd:]
        totals[s] = fold(total, kv, jnp.add)

    def loop(step):
        def one(s, carry):
            step(s)
            return carry
        lax.fori_loop(0, slots, one, 0, unroll=4)

    for s in range(slots):
        k_copy(s).wait()
    loop(score)
    best = jnp.full((group, LANES), LOW, jnp.float32)
    for s in range(slots):
        best = jnp.maximum(best, jnp.where(home == seqs[s], peaks[s], LOW))
    best_own[...] = best
    swap = remote(best_own, best_in, swap_sem.at[0], swap_sem.at[1], partner)
    swap.start()
    for s in range(slots):
        v_copy(s).wait()
    loop(weigh)
    swap.wait()
    best = jnp.maximum(best_own[...], best_in[...])
    total = jnp.zeros((group, LANES), jnp.float32)
    for s in range(slots):
        ours = fold(jnp.where(home == seqs[s], best, LOW), kv, jnp.maximum)
        scale = jnp.exp2(peaks[s] - ours)
        total = total + jnp.where(home == seqs[s], totals[s] * scale, 0.0)
        sums[s] = sums[s] * spread(scale, 0, kv) + sums[before[s]]

    def piece(o, core):
        j = o * 2 + core
        if per == 1:
            return sums[final[j]]
        return sums[final[j // per], pl.ds(pl.multiple_of(j % per * share, share), share), :]

    tot_own[...] = total
    for o in range(outer):
        acc_send[o] = piece(o, 1 - inner).astype(jnp.bfloat16)
    c1 = remote(acc_send, acc_in, swap_sem.at[2], swap_sem.at[3], partner)
    c2 = remote(tot_own, tot_in, swap_sem.at[4], swap_sem.at[5], partner)
    c2.start()
    c1.start()
    c2.wait()
    total = tot_own[...] + tot_in[...]
    stats = []
    for r in range(1, outer + 1):
        o = (mine + r) % outer
        j = o * 2 + inner
        tb = fold(jnp.where(home == j // per, best, LOW), kv, jnp.maximum)
        tt = fold(jnp.where(home == j // per, total, 0.0), kv, jnp.add)
        if per > 1:
            turn = (LANES - j % per * held) % LANES
            tb, tt = pltpu.roll(tb, turn, 1), pltpu.roll(tt, turn, 1)
        stats.append(jnp.where(lane < LANES // 2, tb, tt))
    c1.wait()
    last = []
    for r in range(1, outer + 1):
        o = (mine + r) % outer
        both = (piece(o, inner) + acc_in[o].astype(jnp.float32)).astype(jnp.bfloat16)
        if r == outer:
            acc2_in[o] = both
            stat2_in[o] = stats[r - 1]
            break
        acc2[o] = both
        stat2[o] = stats[r - 1]
        dev = o * 2 + inner
        c1 = remote(acc2.at[o], acc2_in.at[mine], as_sem.at[r - 1], ar_sem.at[mine], dev)
        c2 = remote(stat2.at[o], stat2_in.at[mine], ss_sem.at[r - 1], sr_sem.at[mine], dev)
        c2.start()
        c1.start()
        last += [c1, c2]
    for r in range(1, outer):
        o = (mine + outer - r) % outer
        remote(stat2.at[o], stat2_in.at[o], ss_sem.at[0], sr_sem.at[o], partner).wait_recv()
        remote(acc2.at[o], acc2_in.at[o], as_sem.at[0], ar_sem.at[o], partner).wait_recv()
    pairs = [unpack(stat2_in[o], lane) for o in range(outer)]
    best = pairs[0][0]
    for top, _ in pairs[1:]:
        best = jnp.maximum(best, top)
    scales = [jnp.exp2(top - best) for top, _ in pairs]
    total = scales[0] * pairs[0][1]
    for o in range(1, outer):
        total = total + scales[o] * pairs[o][1]
    out = jnp.zeros((share, hd), jnp.float32)
    for o in range(outer):
        out = out + spread(scales[o] / total, 0, held) * acc2_in[o].astype(jnp.float32)
    out_ref[...] = out.astype(jnp.bfloat16)
    for c in sends + last:
        c.wait_send()


def body(queries, keys, values, lengths, slot_block):
    slots, block, kv, hd = keys.shape
    share = queries.shape[0]
    n = lax.axis_size("seq")
    batch = lengths.shape[0]
    heads = n * share // batch
    group = heads // kv
    outer = n // 2
    cols = block * kv
    assert batch * kv <= LANES
    f32, bf16 = jnp.float32, jnp.bfloat16
    dma = pltpu.SemaphoreType.DMA
    vmem = pl.BlockSpec(memory_space=pltpu.VMEM)
    hbm = pl.BlockSpec(memory_space=pltpu.HBM)
    tile = (group, LANES)
    result = pl.pallas_call(
        functools.partial(kernel, n, batch, block, kv, hd ** (-0.5) * math.log2(math.e)),
        out_shape=jax.ShapeDtypeStruct((share, hd), bf16),
        in_specs=[hbm] * 5,
        out_specs=vmem,
        scratch_shapes=[
            pltpu.SMEM(lengths.shape, jnp.int32),
            pltpu.SMEM(slot_block.shape, jnp.int32),
            pltpu.SMEM((batch,), jnp.int32),
            pltpu.VMEM((share, hd), bf16),
            pltpu.VMEM((n, share, hd), bf16),
            pltpu.VMEM((slots, cols, hd), bf16),
            pltpu.VMEM((slots, cols, hd), bf16),
            pltpu.VMEM((slots, group, cols), f32),
            pltpu.VMEM((slots + 1, heads, hd), f32),
            pltpu.VMEM((slots, *tile), f32),
            pltpu.VMEM((slots, *tile), f32),
            pltpu.VMEM(tile, f32),
            pltpu.VMEM(tile, f32),
            pltpu.VMEM(tile, f32),
            pltpu.VMEM(tile, f32),
            pltpu.VMEM((outer, share, hd), bf16),
            pltpu.VMEM((outer, share, hd), bf16),
            pltpu.VMEM((outer, share, hd), bf16),
            pltpu.VMEM((outer, *tile), f32),
            pltpu.VMEM((outer, share, hd), bf16),
            pltpu.VMEM((outer, *tile), f32),
            dma((slots,)), dma((slots,)), dma, dma((3,)),
            dma((outer,)), dma((n,)), dma((outer,)), dma((6,)),
            dma((outer,)), dma((outer,)), dma((outer,)), dma((outer,)),
        ],
        compiler_params=pltpu.CompilerParams(
            collective_id=0, has_side_effects=True, vmem_limit_bytes=67043328
        ),
        name="decode",
    )(
        lengths,
        slot_block,
        queries.reshape(share, hd),
        keys.reshape(slots, cols, hd),
        values.reshape(slots, cols, hd),
    )
    return result.reshape(share, 1, hd)


def solution(mesh):
    placed = (
        P(("grp", "seq"), "head", None),
        P(("grp", "seq"), None, "head", None),
        P(("grp", "seq"), None, "head", None),
        P("grp"),
        P(("grp", "seq")),
    )
    return jax.shard_map(
        body, mesh=mesh, in_specs=placed, out_specs=P(("grp", "seq"), "head", None), check_vma=False
    )
```

```python
import functools
import math
import jax
import jax.numpy as jnp
from jax import lax
from jax.experimental import pallas as pl
from jax.experimental.pallas import tpu as pltpu
from jax.sharding import PartitionSpec as P

LANES = 128
MESH_ID = pl.DeviceIdType.MESH
LOW = -1e30
DEAD = -3e38


def fold(tile, step, op):
    shift = LANES // 2
    while shift >= step:
        tile = op(tile, pltpu.roll(tile, shift, 1))
        shift //= 2
    return tile


def spread(tile, start, heads):
    group = tile.shape[0]
    return jnp.concatenate(
        [jnp.broadcast_to(tile[:, start + h : start + h + 1], (group, LANES)) for h in range(heads)],
        axis=0,
    )


def kernel(
    n, batch, block, kv, factor,
    lengths_hbm, block_hbm, q_hbm, k_hbm, v_hbm, out_ref,
    lengths, slot_block, final, q_ref, q_all, k_buf, k_turn, v_buf, scores, sums, peaks, totals,
    best_own, best_in, tot_own, tot_in, acc_send, acc_in, mail, mail_in,
    k_sem, v_sem, own_sem, in_sem, qs_sem, qr_sem, fs_sem, swap_sem, as_sem, ar_sem,
):
    slots, cols, hd = k_buf.shape
    share = q_ref.shape[0]
    outer = n // 2
    per = n // batch
    blocks = slots * n // batch
    heads = per * share
    group = heads // kv
    held = share // group
    half = cols // 2
    me = lax.axis_index("seq")
    mine, inner = me // 2, me % 2
    partner = me + 1 - 2 * inner

    def k_copy(s):
        return pltpu.make_async_copy(k_hbm.at[s], k_buf.at[s], k_sem.at[s])

    def v_copy(s):
        return pltpu.make_async_copy(v_hbm.at[s], v_buf.at[s], v_sem.at[s])

    def remote(src, dst, ssem, rsem, dev):
        return pltpu.make_async_remote_copy(
            src_ref=src, dst_ref=dst, send_sem=ssem, recv_sem=rsem,
            device_id={"seq": dev}, device_id_type=MESH_ID,
        )

    q_in = pltpu.make_async_copy(q_hbm, q_ref, in_sem.at[0])
    q_in.start()
    peers = [(mine + r) % outer for r in range(1, outer)]
    barrier = pltpu.get_barrier_semaphore()
    for o in peers:
        pl.semaphore_signal(barrier, inc=1, device_id={"seq": o * 2 + inner}, device_id_type=MESH_ID)
    pl.semaphore_signal(barrier, inc=1, device_id={"seq": partner}, device_id_type=MESH_ID)
    len_in = pltpu.make_async_copy(lengths_hbm, lengths, in_sem.at[1])
    block_in = pltpu.make_async_copy(block_hbm, slot_block, in_sem.at[2])
    len_in.start()
    block_in.start()
    own = pltpu.make_async_copy(q_hbm, q_all.at[me], own_sem)
    own.start()
    for s in range(slots):
        k_copy(s).start()
    sums[...] = jnp.zeros_like(sums)
    len_in.wait()
    block_in.wait()
    seqs = [slot_block[s] // blocks for s in range(slots)]
    before = []
    for s in range(slots):
        prev = slots
        for t in range(s):
            prev = jnp.where(seqs[t] == seqs[s], t, prev)
        before.append(prev)
    for b in range(batch):
        last = slots
        for s in range(slots):
            last = jnp.where(seqs[s] == b, s, last)
        final[b] = last
    q_in.wait()
    chunk = min(half, 512)

    def turn_keys():
        def one(s, carry):
            k_copy(s).wait()
            v_copy(s).start()
            for c in range(0, half, chunk):
                k_turn[s, :hd, c : c + chunk] = k_buf[s, c : c + chunk, :].T
                k_turn[s, hd:, c : c + chunk] = k_buf[s, half + c : half + c + chunk, :].T
            return carry
        lax.fori_loop(0, slots, one, 0)

    early = mine < outer // 2
    pl.when(early)(turn_keys)
    pl.semaphore_wait(barrier, outer)

    sends = []
    for r, o in enumerate(peers):
        sends.append(remote(q_ref, q_all.at[me], qs_sem.at[r], qr_sem.at[me], o * 2 + inner))
    sends.append(remote(q_ref, q_all.at[me], qs_sem.at[outer - 1], qr_sem.at[me], partner))
    for c in sends:
        c.start()
    pl.when(jnp.logical_not(early))(turn_keys)
    for r in range(1, outer):
        src = ((mine + outer - r) % outer) * 2 + inner
        remote(q_ref, q_all.at[src], qs_sem.at[0], qr_sem.at[src], partner).wait_recv()
        c = remote(q_all.at[src], q_all.at[src], fs_sem.at[r - 1], qr_sem.at[src], partner)
        c.start()
        sends.append(c)
    own.wait()
    remote(q_ref, q_all.at[partner], qs_sem.at[0], qr_sem.at[partner], partner).wait_recv()
    for r in range(1, outer):
        src = ((mine + outer - r) % outer) * 2 + 1 - inner
        remote(q_ref, q_all.at[src], qs_sem.at[0], qr_sem.at[src], partner).wait_recv()

    lane = lax.broadcasted_iota(jnp.int32, (group, LANES), 1)
    home = lane // kv
    wide = lax.broadcasted_iota(jnp.int32, (group, chunk), 1)
    picks = [wide % kv == h for h in range(kv)]

    def score(s):
        code = slot_block[s]
        seq, blk = code // blocks, code % blocks
        limit = (lengths[seq] - blk * block) * kv
        q = q_all[pl.ds(seq * per, per)]
        if per > 1:
            q = q.astype(jnp.float32).reshape(heads, hd).astype(jnp.bfloat16)
        else:
            q = q.reshape(heads, hd)
        blank = jnp.zeros_like(q)
        both = jnp.concatenate(
            [jnp.concatenate([q, blank], axis=0), jnp.concatenate([blank, q], axis=0)], axis=1
        )
        top = jnp.full((group, LANES), LOW, jnp.float32)
        for c in range(0, half, chunk):
            full = jnp.dot(both, k_turn[s, :, c : c + chunk], preferred_element_type=jnp.float32)
            for x, at in ((0, c), (heads, half + c)):
                packed = full[x : x + group]
                for h in range(1, kv):
                    packed = jnp.where(picks[h], full[x + h * group : x + (h + 1) * group], packed)
                packed = jnp.where(wide < limit - at, packed * factor, DEAD)
                scores[s, :, at : at + chunk] = packed
                for l in range(0, chunk, LANES):
                    top = jnp.maximum(top, packed[:, l : l + LANES])
        peaks[s] = fold(top, kv, jnp.maximum)

    def weigh(s):
        top = jnp.concatenate([peaks[s]] * (chunk // LANES), axis=1)
        total = jnp.zeros((group, LANES), jnp.float32)
        out = jnp.zeros((2 * heads, 2 * hd), jnp.float32)
        for c in range(0, half, chunk):
            rows = []
            for at in (c, half + c):
                weight = jnp.exp2(scores[s, :, at : at + chunk] - top).astype(jnp.bfloat16)
                weight = weight.astype(jnp.float32)
                for l in range(0, chunk, LANES):
                    total = total + weight[:, l : l + LANES]
                rows += [jnp.where(picks[h], weight, 0.0) for h in range(kv)]
            vals = jnp.concatenate(
                [v_buf[s, c : c + chunk, :], v_buf[s, half + c : half + c + chunk, :]], axis=1
            )
            out = out + jnp.dot(
                jnp.concatenate(rows, axis=0).astype(jnp.bfloat16), vals,
                preferred_element_type=jnp.float32,
            )
        sums[s] = out[:heads, :hd] + out[heads:, hd:]
        totals[s] = fold(total, kv, jnp.add)

    def loop(step):
        def one(s, carry):
            step(s)
            return carry
        lax.fori_loop(0, slots, one, 0, unroll=True)

    loop(score)
    best = jnp.full((group, LANES), LOW, jnp.float32)
    for s in range(slots):
        best = jnp.maximum(best, jnp.where(home == seqs[s], peaks[s], LOW))
    best_own[...] = best
    swap = remote(best_own, best_in, swap_sem.at[0], swap_sem.at[1], partner)
    swap.start()
    for s in range(slots):
        v_copy(s).wait()
    loop(weigh)
    swap.wait()
    best = jnp.maximum(best_own[...], best_in[...])
    total = jnp.zeros((group, LANES), jnp.float32)
    for s in range(slots):
        ours = fold(jnp.where(home == seqs[s], best, LOW), kv, jnp.maximum)
        scale = jnp.exp2(peaks[s] - ours)
        total = total + jnp.where(home == seqs[s], totals[s] * scale, 0.0)
        sums[s] = sums[s] * spread(scale, 0, kv) + sums[before[s]]

    def piece(o, core):
        j = o * 2 + core
        if per == 1:
            return sums[final[j]]
        return sums[final[j // per], pl.ds(pl.multiple_of(j % per * share, share), share), :]

    sub = lax.broadcasted_iota(jnp.int32, (group, LANES), 0)
    diagonal = lane % (LANES // 2) // kv == sub
    tot_own[...] = total
    for o in range(outer):
        acc_send[o] = piece(o, 1 - inner).astype(jnp.bfloat16)
    c1 = remote(acc_send, acc_in, swap_sem.at[2], swap_sem.at[3], partner)
    c2 = remote(tot_own, tot_in, swap_sem.at[4], swap_sem.at[5], partner)
    c2.start()
    c1.start()
    c2.wait()
    total = tot_own[...] + tot_in[...]
    stats = []
    for r in range(1, outer + 1):
        o = (mine + r) % outer
        j = o * 2 + inner
        tb = fold(jnp.where(home == j // per, best, LOW), kv, jnp.maximum)
        tt = fold(jnp.where(home == j // per, total, 0.0), kv, jnp.add)
        if per > 1:
            turn = (LANES - j % per * held) % LANES
            tb, tt = pltpu.roll(tb, turn, 1), pltpu.roll(tt, turn, 1)
        mix = jnp.where(diagonal, jnp.where(lane < LANES // 2, tb, tt), 0.0)
        line = jnp.sum(mix, axis=0, keepdims=True)
        first = line.astype(jnp.bfloat16).astype(jnp.float32)
        second = (line - first).astype(jnp.bfloat16).astype(jnp.float32)
        third = line - first - second
        stats.append(jnp.where(sub == 0, first, jnp.where(sub == 1, second, third)).astype(jnp.bfloat16))
    c1.wait()
    last = []
    for r in range(1, outer + 1):
        o = (mine + r) % outer
        both = (piece(o, inner) + acc_in[o].astype(jnp.float32)).astype(jnp.bfloat16)
        into = mail_in if r == outer else mail
        into[o, :share] = both
        into[o, share:] = stats[r - 1]
        if r < outer:
            c = remote(mail.at[o], mail_in.at[mine], as_sem.at[r - 1], ar_sem.at[mine], o * 2 + inner)
            c.start()
            last.append(c)
    for r in range(1, outer):
        o = (mine + outer - r) % outer
        remote(mail.at[o], mail_in.at[o], as_sem.at[0], ar_sem.at[o], partner).wait_recv()
    tops = []
    for o in range(outer):
        lines = mail_in[o, share:].astype(jnp.float32)
        line = lines[0:1] + lines[1:2] + lines[2:3]
        tile = jnp.where(diagonal, line, 0.0)
        step = kv
        while step < LANES // 2:
            tile = tile + pltpu.roll(tile, step, 1)
            step *= 2
        tops.append(tile)
    best = functools.reduce(jnp.maximum, tops)
    scales = [jnp.exp2(top - best) for top in tops]
    total = sum(scale * pltpu.roll(top, LANES // 2, 1) for scale, top in zip(scales, tops))
    out = jnp.zeros((share, hd), jnp.float32)
    for o in range(outer):
        out = out + spread(scales[o] / total, LANES // 2 - kv, held) * mail_in[o, :share].astype(jnp.float32)
    out_ref[...] = out.astype(jnp.bfloat16)
    for c in sends + last:
        c.wait_send()


def body(queries, keys, values, lengths, slot_block):
    slots, block, kv, hd = keys.shape
    share = queries.shape[0]
    n = lax.axis_size("seq")
    batch = lengths.shape[0]
    heads = n * share // batch
    group = heads // kv
    outer = n // 2
    cols = block * kv
    assert batch * kv <= LANES
    f32, bf16 = jnp.float32, jnp.bfloat16
    dma = pltpu.SemaphoreType.DMA
    vmem = pl.BlockSpec(memory_space=pltpu.VMEM)
    hbm = pl.BlockSpec(memory_space=pltpu.HBM)
    tile = (group, LANES)
    result = pl.pallas_call(
        functools.partial(kernel, n, batch, block, kv, hd ** (-0.5) * math.log2(math.e)),
        out_shape=pltpu.VMEM((share, hd), bf16),
        in_specs=[hbm] * 5,
        out_specs=vmem,
        scratch_shapes=[
            pltpu.SMEM(lengths.shape, jnp.int32),
            pltpu.SMEM(slot_block.shape, jnp.int32),
            pltpu.SMEM((batch,), jnp.int32),
            pltpu.VMEM((share, hd), bf16),
            pltpu.VMEM((n, share, hd), bf16),
            pltpu.VMEM((slots, cols, hd), bf16),
            pltpu.VMEM((slots, 2 * hd, cols // 2), bf16),
            pltpu.VMEM((slots, cols, hd), bf16),
            pltpu.VMEM((slots, group, cols), f32),
            pltpu.VMEM((slots + 1, heads, hd), f32),
            pltpu.VMEM((slots, *tile), f32),
            pltpu.VMEM((slots, *tile), f32),
            pltpu.VMEM(tile, f32),
            pltpu.VMEM(tile, f32),
            pltpu.VMEM(tile, f32),
            pltpu.VMEM(tile, f32),
            pltpu.VMEM((outer, share, hd), bf16),
            pltpu.VMEM((outer, share, hd), bf16),
            pltpu.VMEM((outer, share + group, hd), bf16),
            pltpu.VMEM((outer, share + group, hd), bf16),
            dma((slots,)), dma((slots,)), dma, dma((3,)),
            dma((outer,)), dma((n,)), dma((outer,)), dma((6,)),
            dma((outer,)), dma((outer,)),
        ],
        compiler_params=pltpu.CompilerParams(
            collective_id=0, has_side_effects=True, vmem_limit_bytes=67043328 - max(share * hd * 2, 2**14)
        ),
        name="decode",
    )(
        lengths,
        slot_block,
        queries.reshape(share, hd),
        keys.reshape(slots, cols, hd),
        values.reshape(slots, cols, hd),
    )
    return result.reshape(share, 1, hd)


def solution(mesh):
    placed = (
        P(("grp", "seq"), "head", None),
        P(("grp", "seq"), None, "head", None),
        P(("grp", "seq"), None, "head", None),
        P("grp"),
        P(("grp", "seq")),
    )
    return jax.shard_map(
        body, mesh=mesh, in_specs=placed, out_specs=P(("grp", "seq"), "head", None), check_vma=False
    )
```

```python
import functools
import math
import jax
import jax.numpy as jnp
from jax import lax
from jax.experimental import pallas as pl
from jax.experimental.pallas import tpu as pltpu
from jax.sharding import PartitionSpec as P

LANES = 128
MESH_ID = pl.DeviceIdType.MESH
LOW = -1e30
DEAD = -3e38
PLANE = 2


def fold(tile, step, op):
    shift = LANES // 2
    while shift >= step:
        tile = op(tile, pltpu.roll(tile, shift, 1))
        shift //= 2
    return tile


def spread(tile, start, heads):
    group = tile.shape[0]
    return jnp.concatenate(
        [jnp.broadcast_to(tile[:, start + h : start + h + 1], (group, LANES)) for h in range(heads)],
        axis=0,
    )


def kernel(
    n, batch, block, kv, factor,
    lengths_hbm, block_hbm, q_hbm, k_hbm, v_hbm, out_ref,
    lengths, slot_block, final, q_ref, q_all, k_buf, k_turn, v_buf, scores, sums, peaks, totals,
    best_own, best_in, tot_own, tot_in, acc_send, acc_in, mail, mail_in,
    k_sem, v_sem, own_sem, in_sem, qs_sem, qr_sem, fs_sem, relay_sem, swap_sem, as_sem, ar_sem,
):
    slots, cols, hd = k_buf.shape
    share = q_ref.shape[0]
    outer = n // 2
    per = n // batch
    blocks = slots * n // batch
    heads = per * share
    group = heads // kv
    held = share // group
    half = cols // 2
    me = lax.axis_index("seq")
    mine, inner = me // 2, me % 2
    partner = me + 1 - 2 * inner

    def k_copy(s):
        return pltpu.make_async_copy(k_hbm.at[s], k_buf.at[s], k_sem.at[s])

    def v_copy(s):
        return pltpu.make_async_copy(v_hbm.at[s], v_buf.at[s], v_sem.at[s])

    def remote(src, dst, ssem, rsem, dev):
        return pltpu.make_async_remote_copy(
            src_ref=src, dst_ref=dst, send_sem=ssem, recv_sem=rsem,
            device_id={"seq": dev}, device_id_type=MESH_ID,
        )

    q_in = pltpu.make_async_copy(q_hbm, q_ref, in_sem.at[0])
    q_in.start()
    peers = [(mine + r) % outer for r in range(1, outer)]
    barrier = pltpu.get_barrier_semaphore()
    near = mine < 2 * PLANE
    front, relaying = mine < PLANE, jnp.logical_and(mine >= PLANE, near)

    def greet(o):
        pl.semaphore_signal(barrier, inc=1, device_id={"seq": o * 2 + inner}, device_id_type=MESH_ID)

    for o in peers:
        pl.when(jnp.logical_or(near, o >= PLANE))(functools.partial(greet, o))
    pl.semaphore_signal(barrier, inc=1, device_id={"seq": partner}, device_id_type=MESH_ID)
    len_in = pltpu.make_async_copy(lengths_hbm, lengths, in_sem.at[1])
    block_in = pltpu.make_async_copy(block_hbm, slot_block, in_sem.at[2])
    len_in.start()
    block_in.start()
    own = pltpu.make_async_copy(q_hbm, q_all.at[me], own_sem)
    own.start()
    for s in range(slots):
        k_copy(s).start()
    sums[...] = jnp.zeros_like(sums)
    len_in.wait()
    block_in.wait()
    seqs = [slot_block[s] // blocks for s in range(slots)]
    before = []
    for s in range(slots):
        prev = slots
        for t in range(s):
            prev = jnp.where(seqs[t] == seqs[s], t, prev)
        before.append(prev)
    for b in range(batch):
        last = slots
        for s in range(slots):
            last = jnp.where(seqs[s] == b, s, last)
        final[b] = last
    q_in.wait()
    chunk = min(half, 512)

    def turn_keys():
        def one(s, carry):
            k_copy(s).wait()
            v_copy(s).start()
            for c in range(0, half, chunk):
                k_turn[s, :hd, c : c + chunk] = k_buf[s, c : c + chunk, :].T
                k_turn[s, hd:, c : c + chunk] = k_buf[s, half + c : half + c + chunk, :].T
            return carry
        lax.fori_loop(0, slots, one, 0)

    pl.semaphore_wait(barrier, jnp.where(front, 2 * PLANE, outer))

    direct = []
    for r, o in enumerate(peers):
        c = remote(q_ref, q_all.at[me], qs_sem.at[r], qr_sem.at[me], o * 2 + inner)
        direct.append((jnp.logical_or(jnp.logical_not(front), o < 2 * PLANE), c))
    for asked, c in direct:
        pl.when(asked)(c.start)
    sends = [remote(q_ref, q_all.at[me], qs_sem.at[outer - 1], qr_sem.at[me], partner)]
    sends[0].start()
    origin = (mine + outer - PLANE) % outer * 2 + inner
    relays = [
        remote(q_all.at[origin], q_all.at[origin], relay_sem.at[t], qr_sem.at[origin], (2 * PLANE + t) * 2 + inner)
        for t in range(outer - 2 * PLANE)
    ]

    def hand_on():
        remote(q_ref, q_all.at[origin], qs_sem.at[0], qr_sem.at[origin], partner).wait_recv()
        for c in relays:
            c.start()

    pl.when(relaying)(hand_on)
    turn_keys()
    for r in range(1, outer):
        src = ((mine + outer - r) % outer) * 2 + inner
        arrival = remote(q_ref, q_all.at[src], qs_sem.at[0], qr_sem.at[src], partner)
        if r == PLANE:
            pl.when(jnp.logical_not(relaying))(arrival.wait_recv)
        else:
            arrival.wait_recv()
        c = remote(q_all.at[src], q_all.at[src], fs_sem.at[r - 1], qr_sem.at[src], partner)
        c.start()
        sends.append(c)
    own.wait()
    remote(q_ref, q_all.at[partner], qs_sem.at[0], qr_sem.at[partner], partner).wait_recv()
    for r in range(1, outer):
        src = ((mine + outer - r) % outer) * 2 + 1 - inner
        remote(q_ref, q_all.at[src], qs_sem.at[0], qr_sem.at[src], partner).wait_recv()

    lane = lax.broadcasted_iota(jnp.int32, (group, LANES), 1)
    home = lane // kv
    wide = lax.broadcasted_iota(jnp.int32, (group, chunk), 1)
    picks = [wide % kv == h for h in range(kv)]

    def score(s):
        code = slot_block[s]
        seq, blk = code // blocks, code % blocks
        limit = (lengths[seq] - blk * block) * kv
        q = q_all[pl.ds(seq * per, per)]
        if per > 1:
            q = q.astype(jnp.float32).reshape(heads, hd).astype(jnp.bfloat16)
        else:
            q = q.reshape(heads, hd)
        blank = jnp.zeros_like(q)
        both = jnp.concatenate(
            [jnp.concatenate([q, blank], axis=0), jnp.concatenate([blank, q], axis=0)], axis=1
        )
        top = jnp.full((group, LANES), LOW, jnp.float32)
        for c in range(0, half, chunk):
            full = jnp.dot(both, k_turn[s, :, c : c + chunk], preferred_element_type=jnp.float32)
            for x, at in ((0, c), (heads, half + c)):
                packed = full[x : x + group]
                for h in range(1, kv):
                    packed = jnp.where(picks[h], full[x + h * group : x + (h + 1) * group], packed)
                packed = jnp.where(wide < limit - at, packed * factor, DEAD)
                scores[s, :, at : at + chunk] = packed
                for l in range(0, chunk, LANES):
                    top = jnp.maximum(top, packed[:, l : l + LANES])
        peaks[s] = fold(top, kv, jnp.maximum)

    def weigh(s):
        top = jnp.concatenate([peaks[s]] * (chunk // LANES), axis=1)
        total = jnp.zeros((group, LANES), jnp.float32)
        out = jnp.zeros((2 * heads, 2 * hd), jnp.float32)
        for c in range(0, half, chunk):
            rows = []
            for at in (c, half + c):
                weight = jnp.exp2(scores[s, :, at : at + chunk] - top).astype(jnp.bfloat16)
                weight = weight.astype(jnp.float32)
                for l in range(0, chunk, LANES):
                    total = total + weight[:, l : l + LANES]
                rows += [jnp.where(picks[h], weight, 0.0) for h in range(kv)]
            vals = jnp.concatenate(
                [v_buf[s, c : c + chunk, :], v_buf[s, half + c : half + c + chunk, :]], axis=1
            )
            out = out + jnp.dot(
                jnp.concatenate(rows, axis=0).astype(jnp.bfloat16), vals,
                preferred_element_type=jnp.float32,
            )
        sums[s] = out[:heads, :hd] + out[heads:, hd:]
        totals[s] = fold(total, kv, jnp.add)

    def loop(step):
        def one(s, carry):
            step(s)
            return carry
        lax.fori_loop(0, slots, one, 0, unroll=True)

    loop(score)
    best = jnp.full((group, LANES), LOW, jnp.float32)
    for s in range(slots):
        best = jnp.maximum(best, jnp.where(home == seqs[s], peaks[s], LOW))
    best_own[...] = best
    swap = remote(best_own, best_in, swap_sem.at[0], swap_sem.at[1], partner)
    swap.start()
    for s in range(slots):
        v_copy(s).wait()
    loop(weigh)
    swap.wait()
    best = jnp.maximum(best_own[...], best_in[...])
    total = jnp.zeros((group, LANES), jnp.float32)
    for s in range(slots):
        ours = fold(jnp.where(home == seqs[s], best, LOW), kv, jnp.maximum)
        scale = jnp.exp2(peaks[s] - ours)
        total = total + jnp.where(home == seqs[s], totals[s] * scale, 0.0)
        sums[s] = sums[s] * spread(scale, 0, kv) + sums[before[s]]

    def piece(o, core):
        j = o * 2 + core
        if per == 1:
            return sums[final[j]]
        return sums[final[j // per], pl.ds(pl.multiple_of(j % per * share, share), share), :]

    sub = lax.broadcasted_iota(jnp.int32, (group, LANES), 0)
    diagonal = lane % (LANES // 2) // kv == sub
    tot_own[...] = total
    for o in range(outer):
        acc_send[o] = piece(o, 1 - inner).astype(jnp.bfloat16)
    c1 = remote(acc_send, acc_in, swap_sem.at[2], swap_sem.at[3], partner)
    c2 = remote(tot_own, tot_in, swap_sem.at[4], swap_sem.at[5], partner)
    c2.start()
    c1.start()
    c2.wait()
    total = tot_own[...] + tot_in[...]
    stats = []
    for r in range(1, outer + 1):
        o = (mine + r) % outer
        j = o * 2 + inner
        tb = fold(jnp.where(home == j // per, best, LOW), kv, jnp.maximum)
        tt = fold(jnp.where(home == j // per, total, 0.0), kv, jnp.add)
        if per > 1:
            turn = (LANES - j % per * held) % LANES
            tb, tt = pltpu.roll(tb, turn, 1), pltpu.roll(tt, turn, 1)
        mix = jnp.where(diagonal, jnp.where(lane < LANES // 2, tb, tt), 0.0)
        line = jnp.sum(mix, axis=0, keepdims=True)
        first = line.astype(jnp.bfloat16).astype(jnp.float32)
        second = (line - first).astype(jnp.bfloat16).astype(jnp.float32)
        third = line - first - second
        stats.append(jnp.where(sub == 0, first, jnp.where(sub == 1, second, third)).astype(jnp.bfloat16))
    c1.wait()
    last = []
    for r in range(1, outer + 1):
        o = (mine + r) % outer
        both = (piece(o, inner) + acc_in[o].astype(jnp.float32)).astype(jnp.bfloat16)
        into = mail_in if r == outer else mail
        into[o, :share] = both
        into[o, share:] = stats[r - 1]
        if r < outer:
            c = remote(mail.at[o], mail_in.at[mine], as_sem.at[r - 1], ar_sem.at[mine], o * 2 + inner)
            c.start()
            last.append(c)
    for r in range(1, outer):
        o = (mine + outer - r) % outer
        remote(mail.at[o], mail_in.at[o], as_sem.at[0], ar_sem.at[o], partner).wait_recv()
    tops = []
    for o in range(outer):
        lines = mail_in[o, share:].astype(jnp.float32)
        line = lines[0:1] + lines[1:2] + lines[2:3]
        tile = jnp.where(diagonal, line, 0.0)
        step = kv
        while step < LANES // 2:
            tile = tile + pltpu.roll(tile, step, 1)
            step *= 2
        tops.append(tile)
    best = functools.reduce(jnp.maximum, tops)
    scales = [jnp.exp2(top - best) for top in tops]
    total = sum(scale * pltpu.roll(top, LANES // 2, 1) for scale, top in zip(scales, tops))
    out = jnp.zeros((share, hd), jnp.float32)
    for o in range(outer):
        out = out + spread(scales[o] / total, LANES // 2 - kv, held) * mail_in[o, :share].astype(jnp.float32)
    out_ref[...] = out.astype(jnp.bfloat16)
    for c in sends + last:
        c.wait_send()
    for asked, c in direct:
        pl.when(asked)(c.wait_send)

    def handed_on():
        for c in relays:
            c.wait_send()

    pl.when(relaying)(handed_on)


def body(queries, keys, values, lengths, slot_block):
    slots, block, kv, hd = keys.shape
    share = queries.shape[0]
    n = lax.axis_size("seq")
    batch = lengths.shape[0]
    heads = n * share // batch
    group = heads // kv
    outer = n // 2
    cols = block * kv
    assert batch * kv <= LANES
    f32, bf16 = jnp.float32, jnp.bfloat16
    dma = pltpu.SemaphoreType.DMA
    vmem = pl.BlockSpec(memory_space=pltpu.VMEM)
    hbm = pl.BlockSpec(memory_space=pltpu.HBM)
    tile = (group, LANES)
    result = pl.pallas_call(
        functools.partial(kernel, n, batch, block, kv, hd ** (-0.5) * math.log2(math.e)),
        out_shape=pltpu.VMEM((share, hd), bf16),
        in_specs=[hbm] * 5,
        out_specs=vmem,
        scratch_shapes=[
            pltpu.SMEM(lengths.shape, jnp.int32),
            pltpu.SMEM(slot_block.shape, jnp.int32),
            pltpu.SMEM((batch,), jnp.int32),
            pltpu.VMEM((share, hd), bf16),
            pltpu.VMEM((n, share, hd), bf16),
            pltpu.VMEM((slots, cols, hd), bf16),
            pltpu.VMEM((slots, 2 * hd, cols // 2), bf16),
            pltpu.VMEM((slots, cols, hd), bf16),
            pltpu.VMEM((slots, group, cols), f32),
            pltpu.VMEM((slots + 1, heads, hd), f32),
            pltpu.VMEM((slots, *tile), f32),
            pltpu.VMEM((slots, *tile), f32),
            pltpu.VMEM(tile, f32),
            pltpu.VMEM(tile, f32),
            pltpu.VMEM(tile, f32),
            pltpu.VMEM(tile, f32),
            pltpu.VMEM((outer, share, hd), bf16),
            pltpu.VMEM((outer, share, hd), bf16),
            pltpu.VMEM((outer, share + group, hd), bf16),
            pltpu.VMEM((outer, share + group, hd), bf16),
            dma((slots,)), dma((slots,)), dma, dma((3,)),
            dma((outer,)), dma((n,)), dma((outer,)), dma((outer,)), dma((6,)),
            dma((outer,)), dma((outer,)),
        ],
        compiler_params=pltpu.CompilerParams(
            collective_id=0, has_side_effects=True, vmem_limit_bytes=67043328 - max(share * hd * 2, 2**14)
        ),
        name="decode",
    )(
        lengths,
        slot_block,
        queries.reshape(share, hd),
        keys.reshape(slots, cols, hd),
        values.reshape(slots, cols, hd),
    )
    return result.reshape(share, 1, hd)


def solution(mesh):
    placed = (
        P(("grp", "seq"), "head", None),
        P(("grp", "seq"), None, "head", None),
        P(("grp", "seq"), None, "head", None),
        P("grp"),
        P(("grp", "seq")),
    )
    return jax.shard_map(
        body, mesh=mesh, in_specs=placed, out_specs=P(("grp", "seq"), "head", None), check_vma=False
    )
```

```python
import functools
import math
import jax
import jax.numpy as jnp
from jax import lax
from jax.experimental import pallas as pl
from jax.experimental.pallas import tpu as pltpu
from jax.sharding import PartitionSpec as P

LANES = 128
MESH_ID = pl.DeviceIdType.MESH
LOW = -1e30
DEAD = -3e38
PLANE = 2
LATE = 4


def fold(tile, step, op):
    shift = LANES // 2
    while shift >= step:
        tile = op(tile, pltpu.roll(tile, shift, 1))
        shift //= 2
    return tile


def spread(tile, start, heads):
    group = tile.shape[0]
    return jnp.concatenate(
        [jnp.broadcast_to(tile[:, start + h : start + h + 1], (group, LANES)) for h in range(heads)],
        axis=0,
    )


def kernel(
    n, batch, block, kv, factor,
    lengths_hbm, block_hbm, q_hbm, k_hbm, v_hbm, out_ref,
    lengths, slot_block, final, q_ref, q_all, k_buf, k_turn, v_buf, scores, sums, peaks, totals,
    best_own, best_in, tot_own, tot_in, acc_send, acc_in, mail, mail_in,
    k_sem, v_sem, own_sem, in_sem, qs_sem, qr_sem, fs_sem, relay_sem, swap_sem, as_sem, ar_sem,
):
    slots, cols, hd = k_buf.shape
    share = q_ref.shape[0]
    outer = n // 2
    per = n // batch
    blocks = slots * n // batch
    heads = per * share
    group = heads // kv
    held = share // group
    half = cols // 2
    lead = slots - slots // LATE
    me = lax.axis_index("seq")
    mine, inner = me // 2, me % 2
    other = 1 - inner
    partner = me + 1 - 2 * inner

    def k_copy(s):
        return pltpu.make_async_copy(k_hbm.at[s], k_buf.at[s], k_sem.at[s])

    def v_copy(s):
        return pltpu.make_async_copy(v_hbm.at[s], v_buf.at[s], v_sem.at[s])

    def remote(src, dst, ssem, rsem, dev):
        return pltpu.make_async_remote_copy(
            src_ref=src, dst_ref=dst, send_sem=ssem, recv_sem=rsem,
            device_id={"seq": dev}, device_id_type=MESH_ID,
        )

    q_in = pltpu.make_async_copy(q_hbm, q_ref, in_sem.at[0])
    q_in.start()
    front, relaying = mine < PLANE, jnp.logical_and(mine >= PLANE, mine < 2 * PLANE)
    peers = [(mine + jnp.where(relaying, outer - r, r)) % outer for r in range(1, outer)]
    barrier = pltpu.get_barrier_semaphore()

    def greet(o):
        pl.semaphore_signal(barrier, inc=1, device_id={"seq": o * 2 + other}, device_id_type=MESH_ID)

    for o in peers:
        pl.when(front | (o >= PLANE) | (o + PLANE == mine))(functools.partial(greet, o))
    pl.semaphore_signal(barrier, inc=1, device_id={"seq": partner}, device_id_type=MESH_ID)
    len_in = pltpu.make_async_copy(lengths_hbm, lengths, in_sem.at[1])
    block_in = pltpu.make_async_copy(block_hbm, slot_block, in_sem.at[2])
    len_in.start()
    block_in.start()
    own = pltpu.make_async_copy(q_hbm, q_all.at[me], own_sem)
    own.start()
    for s in range(slots):
        k_copy(s).start()
    for s in range(slots):
        v_copy(s).start(priority=1)
    q_in.wait()
    chunk = min(half, 512)

    def turn_keys():
        def one(s, carry):
            k_copy(s).wait()
            for c in range(0, half, chunk):
                k_turn[s, :hd, c : c + chunk] = k_buf[s, c : c + chunk, :].T
                k_turn[s, hd:, c : c + chunk] = k_buf[s, half + c : half + c + chunk, :].T
            return carry
        lax.fori_loop(0, slots, one, 0)

    pl.semaphore_wait(barrier, jnp.where(front, PLANE + 1, outer))

    direct = []
    for r, o in enumerate(peers):
        c = remote(q_ref, q_all.at[me], qs_sem.at[r], qr_sem.at[me], o * 2 + other)
        direct.append((jnp.logical_not(front) | (o < PLANE) | (o == mine + PLANE), c))
    for asked, c in direct[: outer // 2]:
        pl.when(asked)(c.start)
    sends = [remote(q_ref, q_all.at[me], qs_sem.at[outer - 1], qr_sem.at[me], partner)]
    sends[0].start()
    origin = (mine + outer - PLANE) % outer * 2 + other
    targets = [outer - 1 - t for t in range(outer - 2 * PLANE)]
    targets += [PLANE + (mine + t) % PLANE for t in range(1, PLANE)]
    relays = [
        remote(q_all.at[origin], q_all.at[origin], relay_sem.at[t], qr_sem.at[origin], o * 2 + other)
        for t, o in enumerate(targets)
    ]

    def hand_on():
        remote(q_ref, q_all.at[origin], qs_sem.at[0], qr_sem.at[origin], partner).wait_recv()
        for c in relays:
            c.start()

    def side(o):
        return jnp.where(jnp.logical_not(front) & (o < PLANE) & (o + PLANE != mine), inner, other)

    pl.when(relaying)(hand_on)
    for asked, c in direct[outer // 2 :]:
        pl.when(asked)(c.start)
    sums[...] = jnp.zeros_like(sums)
    len_in.wait()
    block_in.wait()
    seqs = [slot_block[s] // blocks for s in range(slots)]
    before = []
    for s in range(slots):
        prev = slots
        for t in range(s):
            prev = jnp.where(seqs[t] == seqs[s], t, prev)
        before.append(prev)
    for b in range(batch):
        last = slots
        for s in range(slots):
            last = jnp.where(seqs[s] == b, s, last)
        final[b] = last
    turn_keys()
    for r in range(1, outer):
        o = (mine + outer - r) % outer
        src = o * 2 + side(o)
        arrival = remote(q_ref, q_all.at[src], qs_sem.at[0], qr_sem.at[src], partner)
        if r == PLANE:
            pl.when(jnp.logical_not(relaying))(arrival.wait_recv)
        else:
            arrival.wait_recv()
        c = remote(q_all.at[src], q_all.at[src], fs_sem.at[r - 1], qr_sem.at[src], partner)
        c.start()
        sends.append(c)
    own.wait()
    remote(q_ref, q_all.at[partner], qs_sem.at[0], qr_sem.at[partner], partner).wait_recv()
    for r in range(1, outer):
        o = (mine + outer - r) % outer
        src = o * 2 + 1 - side(o)
        remote(q_ref, q_all.at[src], qs_sem.at[0], qr_sem.at[src], partner).wait_recv()

    lane = lax.broadcasted_iota(jnp.int32, (group, LANES), 1)
    home = lane // kv
    wide = lax.broadcasted_iota(jnp.int32, (group, chunk), 1)
    picks = [wide % kv == h for h in range(kv)]

    def score(s):
        code = slot_block[s]
        seq, blk = code // blocks, code % blocks
        limit = (lengths[seq] - blk * block) * kv
        q = q_all[pl.ds(seq * per, per)]
        if per > 1:
            q = q.astype(jnp.float32).reshape(heads, hd).astype(jnp.bfloat16)
        else:
            q = q.reshape(heads, hd)
        blank = jnp.zeros_like(q)
        both = jnp.concatenate(
            [jnp.concatenate([q, blank], axis=0), jnp.concatenate([blank, q], axis=0)], axis=1
        )
        top = jnp.full((group, LANES), LOW, jnp.float32)
        for c in range(0, half, chunk):
            full = jnp.dot(both, k_turn[s, :, c : c + chunk], preferred_element_type=jnp.float32)
            for x, at in ((0, c), (heads, half + c)):
                packed = full[x : x + group]
                for h in range(1, kv):
                    packed = jnp.where(picks[h], full[x + h * group : x + (h + 1) * group], packed)
                packed = jnp.where(wide < limit - at, packed * factor, DEAD)
                scores[s, :, at : at + chunk] = packed
                for l in range(0, chunk, LANES):
                    top = jnp.maximum(top, packed[:, l : l + LANES])
        peaks[s] = fold(top, kv, jnp.maximum)

    def weigh(s):
        top = jnp.concatenate([peaks[s]] * (chunk // LANES), axis=1)
        total = jnp.zeros((group, LANES), jnp.float32)
        out = jnp.zeros((2 * heads, 2 * hd), jnp.float32)
        for c in range(0, half, chunk):
            rows = []
            for at in (c, half + c):
                weight = jnp.exp2(scores[s, :, at : at + chunk] - top).astype(jnp.bfloat16)
                weight = weight.astype(jnp.float32)
                for l in range(0, chunk, LANES):
                    total = total + weight[:, l : l + LANES]
                rows += [jnp.where(picks[h], weight, 0.0) for h in range(kv)]
            vals = jnp.concatenate(
                [v_buf[s, c : c + chunk, :], v_buf[s, half + c : half + c + chunk, :]], axis=1
            )
            out = out + jnp.dot(
                jnp.concatenate(rows, axis=0).astype(jnp.bfloat16), vals,
                preferred_element_type=jnp.float32,
            )
        sums[s] = out[:heads, :hd] + out[heads:, hd:]
        totals[s] = fold(total, kv, jnp.add)

    def loop(step, end):
        def one(s, carry):
            step(s)
            return carry
        lax.fori_loop(0, end, one, 0, unroll=True)

    loop(score, slots)
    best = jnp.full((group, LANES), LOW, jnp.float32)
    for s in range(slots):
        best = jnp.maximum(best, jnp.where(home == seqs[s], peaks[s], LOW))
    best_own[...] = best
    swap = remote(best_own, best_in, swap_sem.at[0], swap_sem.at[1], partner)
    swap.start()
    for s in range(slots):
        v_copy(s).wait()
    loop(weigh, lead)
    swap.wait()
    best = jnp.maximum(best_own[...], best_in[...])

    def gather(s, total):
        ours = fold(jnp.where(home == seqs[s], best, LOW), kv, jnp.maximum)
        scale = jnp.exp2(peaks[s] - ours)
        sums[s] = sums[s] * spread(scale, 0, kv) + sums[before[s]]
        return total + jnp.where(home == seqs[s], totals[s] * scale, 0.0)

    total = jnp.zeros((group, LANES), jnp.float32)
    done = 0
    for s in range(lead, slots):
        weigh(s)
        upto = lead * (s + 1 - lead) // (slots - lead)
        for t in range(done, upto):
            total = gather(t, total)
        done = upto
    for t in range(done, slots):
        total = gather(t, total)

    def piece(o, core):
        j = o * 2 + core
        if per == 1:
            return sums[final[j]]
        return sums[final[j // per], pl.ds(pl.multiple_of(j % per * share, share), share), :]

    sub = lax.broadcasted_iota(jnp.int32, (group, LANES), 0)
    diagonal = lane % (LANES // 2) // kv == sub
    tot_own[...] = total
    for o in range(outer):
        acc_send[o] = piece(o, inner).astype(jnp.bfloat16)
    c1 = remote(acc_send, acc_in, swap_sem.at[2], swap_sem.at[3], partner)
    c2 = remote(tot_own, tot_in, swap_sem.at[4], swap_sem.at[5], partner)
    c2.start()
    c1.start()
    c2.wait()
    total = tot_own[...] + tot_in[...]
    stats = []
    for r in range(1, outer + 1):
        o = (mine + r) % outer
        j = o * 2 + other
        tb = fold(jnp.where(home == j // per, best, LOW), kv, jnp.maximum)
        tt = fold(jnp.where(home == j // per, total, 0.0), kv, jnp.add)
        if per > 1:
            turn = (LANES - j % per * held) % LANES
            tb, tt = pltpu.roll(tb, turn, 1), pltpu.roll(tt, turn, 1)
        mix = jnp.where(diagonal, jnp.where(lane < LANES // 2, tb, tt), 0.0)
        line = jnp.sum(mix, axis=0, keepdims=True)
        first = line.astype(jnp.bfloat16).astype(jnp.float32)
        second = (line - first).astype(jnp.bfloat16).astype(jnp.float32)
        third = line - first - second
        stats.append(jnp.where(sub == 0, first, jnp.where(sub == 1, second, third)).astype(jnp.bfloat16))
    c1.wait()
    last = []
    for r in range(1, outer + 1):
        o = (mine + r) % outer
        both = (piece(o, other) + acc_in[o].astype(jnp.float32)).astype(jnp.bfloat16)
        mail[o, :share] = both
        mail[o, share:] = stats[r - 1]
        c = remote(mail.at[o], mail_in.at[mine], as_sem.at[r - 1], ar_sem.at[mine], o * 2 + other)
        c.start()
        last.append(c)
    for o in range(outer):
        remote(mail.at[o], mail_in.at[o], as_sem.at[0], ar_sem.at[o], partner).wait_recv()
    tops = []
    for o in range(outer):
        lines = mail_in[o, share:].astype(jnp.float32)
        line = lines[0:1] + lines[1:2] + lines[2:3]
        tile = jnp.where(diagonal, line, 0.0)
        step = kv
        while step < LANES // 2:
            tile = tile + pltpu.roll(tile, step, 1)
            step *= 2
        tops.append(tile)
    best = functools.reduce(jnp.maximum, tops)
    scales = [jnp.exp2(top - best) for top in tops]
    total = sum(scale * pltpu.roll(top, LANES // 2, 1) for scale, top in zip(scales, tops))
    out = jnp.zeros((share, hd), jnp.float32)
    for o in range(outer):
        out = out + spread(scales[o] / total, LANES // 2 - kv, held) * mail_in[o, :share].astype(jnp.float32)
    out_ref[...] = out.astype(jnp.bfloat16)
    for c in sends + last:
        c.wait_send()
    for asked, c in direct:
        pl.when(asked)(c.wait_send)

    def handed_on():
        for c in relays:
            c.wait_send()

    pl.when(relaying)(handed_on)


def body(queries, keys, values, lengths, slot_block):
    slots, block, kv, hd = keys.shape
    share = queries.shape[0]
    n = lax.axis_size("seq")
    batch = lengths.shape[0]
    heads = n * share // batch
    group = heads // kv
    outer = n // 2
    cols = block * kv
    assert batch * kv <= LANES
    f32, bf16 = jnp.float32, jnp.bfloat16
    dma = pltpu.SemaphoreType.DMA
    vmem = pl.BlockSpec(memory_space=pltpu.VMEM)
    hbm = pl.BlockSpec(memory_space=pltpu.HBM)
    tile = (group, LANES)
    result = pl.pallas_call(
        functools.partial(kernel, n, batch, block, kv, hd ** (-0.5) * math.log2(math.e)),
        out_shape=pltpu.VMEM((share, hd), bf16),
        in_specs=[hbm] * 5,
        out_specs=vmem,
        scratch_shapes=[
            pltpu.SMEM(lengths.shape, jnp.int32),
            pltpu.SMEM(slot_block.shape, jnp.int32),
            pltpu.SMEM((batch,), jnp.int32),
            pltpu.VMEM((share, hd), bf16),
            pltpu.VMEM((n, share, hd), bf16),
            pltpu.VMEM((slots, cols, hd), bf16),
            pltpu.VMEM((slots, 2 * hd, cols // 2), bf16),
            pltpu.VMEM((slots, cols, hd), bf16),
            pltpu.VMEM((slots, group, cols), f32),
            pltpu.VMEM((slots + 1, heads, hd), f32),
            pltpu.VMEM((slots, *tile), f32),
            pltpu.VMEM((slots, *tile), f32),
            pltpu.VMEM(tile, f32),
            pltpu.VMEM(tile, f32),
            pltpu.VMEM(tile, f32),
            pltpu.VMEM(tile, f32),
            pltpu.VMEM((outer, share, hd), bf16),
            pltpu.VMEM((outer, share, hd), bf16),
            pltpu.VMEM((outer, share + group, hd), bf16),
            pltpu.VMEM((outer, share + group, hd), bf16),
            dma((slots,)), dma((slots,)), dma, dma((3,)),
            dma((outer,)), dma((n,)), dma((outer,)), dma((outer,)), dma((6,)),
            dma((outer,)), dma((outer,)),
        ],
        compiler_params=pltpu.CompilerParams(
            collective_id=0, has_side_effects=True, vmem_limit_bytes=67043328 - max(share * hd * 2, 2**14)
        ),
        name="decode",
    )(
        lengths,
        slot_block,
        queries.reshape(share, hd),
        keys.reshape(slots, cols, hd),
        values.reshape(slots, cols, hd),
    )
    return result.reshape(share, 1, hd)


def solution(mesh):
    placed = (
        P(("grp", "seq"), "head", None),
        P(("grp", "seq"), None, "head", None),
        P(("grp", "seq"), None, "head", None),
        P("grp"),
        P(("grp", "seq")),
    )
    return jax.shard_map(
        body, mesh=mesh, in_specs=placed, out_specs=P(("grp", "seq"), "head", None), check_vma=False
    )
```

```python
import functools
import math
import jax
import jax.numpy as jnp
from jax import lax
from jax.experimental import pallas as pl
from jax.experimental.pallas import tpu as pltpu
from jax.sharding import PartitionSpec as P

LANES = 128
MESH_ID = pl.DeviceIdType.MESH
LOW = -1e30
DEAD = -3e38
PLANE = 2
LATE = 4


def fold(tile, step, op):
    shift = LANES // 2
    while shift >= step:
        tile = op(tile, pltpu.roll(tile, shift, 1))
        shift //= 2
    return tile


def spread(tile, start, heads):
    group = tile.shape[0]
    return jnp.concatenate(
        [jnp.broadcast_to(tile[:, start + h : start + h + 1], (group, LANES)) for h in range(heads)],
        axis=0,
    )


def kernel(
    n, batch, block, kv, factor,
    lengths_hbm, block_hbm, q_hbm, k_hbm, v_hbm, out_ref,
    lengths, slot_block, final, q_ref, q_all, k_buf, k_turn, v_buf, scores, sums, peaks, totals,
    best_own, best_in, tot_own, tot_in, acc_send, acc_in, mail, mail_in,
    k_sem, v_sem, own_sem, in_sem, qs_sem, qr_sem, fs_sem, relay_sem, ready, swap_sem, as_sem, ar_sem,
):
    slots, cols, hd = k_buf.shape
    share = q_ref.shape[0]
    outer = n // 2
    per = n // batch
    blocks = slots * n // batch
    heads = per * share
    group = heads // kv
    held = share // group
    half = cols // 2
    lead = slots - slots // LATE
    me = lax.axis_index("seq")
    mine, inner = me // 2, me % 2
    other = 1 - inner
    partner = me + 1 - 2 * inner

    def k_copy(s):
        return pltpu.make_async_copy(k_hbm.at[s], k_buf.at[s], k_sem.at[s])

    def v_copy(s):
        return pltpu.make_async_copy(v_hbm.at[s], v_buf.at[s], v_sem.at[s])

    def remote(src, dst, ssem, rsem, dev):
        return pltpu.make_async_remote_copy(
            src_ref=src, dst_ref=dst, send_sem=ssem, recv_sem=rsem,
            device_id={"seq": dev}, device_id_type=MESH_ID,
        )

    q_in = pltpu.make_async_copy(q_hbm, q_ref, in_sem.at[0])
    q_in.start()
    edge = outer - PLANE
    late = mine >= edge
    front, relaying = mine < PLANE, jnp.logical_and(mine >= PLANE, mine < 2 * PLANE)
    peers = [(mine + jnp.where(relaying, outer - r, r)) % outer for r in range(1, outer)]
    barrier = pltpu.get_barrier_semaphore()

    def greet(o):
        pl.semaphore_signal(barrier, inc=1, device_id={"seq": o * 2 + other}, device_id_type=MESH_ID)

    for o in peers:
        asks = jnp.where(late, o >= edge, front | (o >= PLANE) | (o + PLANE == mine))
        pl.when(asks)(functools.partial(greet, o))
    pl.semaphore_signal(barrier, inc=1, device_id={"seq": partner}, device_id_type=MESH_ID)
    len_in = pltpu.make_async_copy(lengths_hbm, lengths, in_sem.at[1])
    block_in = pltpu.make_async_copy(block_hbm, slot_block, in_sem.at[2])
    len_in.start()
    block_in.start()
    own = pltpu.make_async_copy(q_hbm, q_all.at[me], own_sem)
    own.start()
    for s in range(slots):
        k_copy(s).start()
    for s in range(slots):
        v_copy(s).start(priority=1)
    q_in.wait()
    chunk = min(half, 512)

    def turn_keys():
        def one(s, carry):
            k_copy(s).wait()
            for c in range(0, half, chunk):
                k_turn[s, :hd, c : c + chunk] = k_buf[s, c : c + chunk, :].T
                k_turn[s, hd:, c : c + chunk] = k_buf[s, half + c : half + c + chunk, :].T
            return carry
        lax.fori_loop(0, slots, one, 0)

    pl.semaphore_wait(barrier, jnp.where(front, PLANE + 1, jnp.where(late, outer, edge)))

    def announce():
        for o in range(PLANE, edge):
            pl.semaphore_signal(ready, inc=1, device_id={"seq": o * 2 + other}, device_id_type=MESH_ID)

    pl.when(late)(announce)
    direct = []
    for r, o in enumerate(peers):
        c = remote(q_ref, q_all.at[me], qs_sem.at[r], qr_sem.at[me], o * 2 + other)
        asked = jnp.logical_not(front) | (o < PLANE) | (o == mine + PLANE)
        direct.append((asked, late | (o < edge), c))
    for asked, soon, c in direct:
        pl.when(asked & soon)(c.start)
    sends = [remote(q_ref, q_all.at[me], qs_sem.at[outer - 1], qr_sem.at[me], partner)]
    sends[0].start()
    origin = (mine + outer - PLANE) % outer * 2 + other
    targets = [edge + t for t in range(PLANE)]
    targets += [PLANE + (mine + t) % PLANE for t in range(1, PLANE)]
    targets += [edge - 1 - t for t in range(edge - 2 * PLANE)]
    relays = [
        remote(q_all.at[origin], q_all.at[origin], relay_sem.at[t], qr_sem.at[origin], o * 2 + other)
        for t, o in enumerate(targets)
    ]

    def receive_first():
        remote(q_ref, q_all.at[origin], qs_sem.at[0], qr_sem.at[origin], partner).wait_recv()
        for c in relays[PLANE : 2 * PLANE - 1]:
            c.start()

    def hand_on():
        for c in relays[:PLANE]:
            c.start()

    def hand_back():
        for c in relays[2 * PLANE - 1 :]:
            c.start()

    def side(o):
        return jnp.where(jnp.logical_not(front) & (o < PLANE) & (o + PLANE != mine), inner, other)

    pl.when(relaying)(receive_first)

    def wait_late():
        pl.semaphore_wait(ready, PLANE)

    pl.when(relaying)(hand_back)
    pl.when(jnp.logical_not(front | late))(wait_late)
    pl.when(relaying)(hand_on)
    for asked, soon, c in direct:
        pl.when(asked & jnp.logical_not(soon))(c.start)
    sums[...] = jnp.zeros_like(sums)
    len_in.wait()
    block_in.wait()
    seqs = [slot_block[s] // blocks for s in range(slots)]
    before = []
    for s in range(slots):
        prev = slots
        for t in range(s):
            prev = jnp.where(seqs[t] == seqs[s], t, prev)
        before.append(prev)
    for b in range(batch):
        last = slots
        for s in range(slots):
            last = jnp.where(seqs[s] == b, s, last)
        final[b] = last
    turn_keys()
    for r in range(1, outer):
        o = (mine + outer - r) % outer
        src = o * 2 + side(o)
        arrival = remote(q_ref, q_all.at[src], qs_sem.at[0], qr_sem.at[src], partner)
        if r == PLANE:
            pl.when(jnp.logical_not(relaying))(arrival.wait_recv)
        else:
            arrival.wait_recv()
        c = remote(q_all.at[src], q_all.at[src], fs_sem.at[r - 1], qr_sem.at[src], partner)
        c.start()
        sends.append(c)
    own.wait()
    remote(q_ref, q_all.at[partner], qs_sem.at[0], qr_sem.at[partner], partner).wait_recv()
    for r in range(1, outer):
        o = (mine + outer - r) % outer
        src = o * 2 + 1 - side(o)
        remote(q_ref, q_all.at[src], qs_sem.at[0], qr_sem.at[src], partner).wait_recv()

    lane = lax.broadcasted_iota(jnp.int32, (group, LANES), 1)
    home = lane // kv
    wide = lax.broadcasted_iota(jnp.int32, (group, chunk), 1)
    picks = [wide % kv == h for h in range(kv)]

    def score(s):
        code = slot_block[s]
        seq, blk = code // blocks, code % blocks
        limit = (lengths[seq] - blk * block) * kv
        q = q_all[pl.ds(seq * per, per)]
        if per > 1:
            q = q.astype(jnp.float32).reshape(heads, hd).astype(jnp.bfloat16)
        else:
            q = q.reshape(heads, hd)
        blank = jnp.zeros_like(q)
        both = jnp.concatenate(
            [jnp.concatenate([q, blank], axis=0), jnp.concatenate([blank, q], axis=0)], axis=1
        )
        top = jnp.full((group, LANES), LOW, jnp.float32)
        for c in range(0, half, chunk):
            full = jnp.dot(both, k_turn[s, :, c : c + chunk], preferred_element_type=jnp.float32)
            for x, at in ((0, c), (heads, half + c)):
                packed = full[x : x + group]
                for h in range(1, kv):
                    packed = jnp.where(picks[h], full[x + h * group : x + (h + 1) * group], packed)
                packed = jnp.where(wide < limit - at, packed * factor, DEAD)
                scores[s, :, at : at + chunk] = packed
                for l in range(0, chunk, LANES):
                    top = jnp.maximum(top, packed[:, l : l + LANES])
        peaks[s] = fold(top, kv, jnp.maximum)

    def weigh(s):
        top = jnp.concatenate([peaks[s]] * (chunk // LANES), axis=1)
        total = jnp.zeros((group, LANES), jnp.float32)
        out = jnp.zeros((2 * heads, 2 * hd), jnp.float32)
        for c in range(0, half, chunk):
            rows = []
            for at in (c, half + c):
                weight = jnp.exp2(scores[s, :, at : at + chunk] - top).astype(jnp.bfloat16)
                weight = weight.astype(jnp.float32)
                for l in range(0, chunk, LANES):
                    total = total + weight[:, l : l + LANES]
                rows += [jnp.where(picks[h], weight, 0.0) for h in range(kv)]
            vals = jnp.concatenate(
                [v_buf[s, c : c + chunk, :], v_buf[s, half + c : half + c + chunk, :]], axis=1
            )
            out = out + jnp.dot(
                jnp.concatenate(rows, axis=0).astype(jnp.bfloat16), vals,
                preferred_element_type=jnp.float32,
            )
        sums[s] = out[:heads, :hd] + out[heads:, hd:]
        totals[s] = fold(total, kv, jnp.add)

    def loop(step, end):
        def one(s, carry):
            step(s)
            return carry
        lax.fori_loop(0, end, one, 0, unroll=True)

    loop(score, slots)
    best = jnp.full((group, LANES), LOW, jnp.float32)
    for s in range(slots):
        best = jnp.maximum(best, jnp.where(home == seqs[s], peaks[s], LOW))
    best_own[...] = best
    swap = remote(best_own, best_in, swap_sem.at[0], swap_sem.at[1], partner)
    swap.start()
    for s in range(slots):
        v_copy(s).wait()
    loop(weigh, lead)
    swap.wait()
    best = jnp.maximum(best_own[...], best_in[...])

    def gather(s, total):
        ours = fold(jnp.where(home == seqs[s], best, LOW), kv, jnp.maximum)
        scale = jnp.exp2(peaks[s] - ours)
        sums[s] = sums[s] * spread(scale, 0, kv) + sums[before[s]]
        return total + jnp.where(home == seqs[s], totals[s] * scale, 0.0)

    total = jnp.zeros((group, LANES), jnp.float32)
    done = 0
    for s in range(lead, slots):
        weigh(s)
        upto = lead * (s + 1 - lead) // (slots - lead)
        for t in range(done, upto):
            total = gather(t, total)
        done = upto
    for t in range(done, slots):
        total = gather(t, total)

    def piece(o, core):
        j = o * 2 + core
        if per == 1:
            return sums[final[j]]
        return sums[final[j // per], pl.ds(pl.multiple_of(j % per * share, share), share), :]

    sub = lax.broadcasted_iota(jnp.int32, (group, LANES), 0)
    diagonal = lane % (LANES // 2) // kv == sub
    tot_own[...] = total
    for o in range(outer):
        acc_send[o] = piece(o, inner).astype(jnp.bfloat16)
    c1 = remote(acc_send, acc_in, swap_sem.at[2], swap_sem.at[3], partner)
    c2 = remote(tot_own, tot_in, swap_sem.at[4], swap_sem.at[5], partner)
    c2.start()
    c1.start()
    c2.wait()
    total = tot_own[...] + tot_in[...]
    stats = []
    for r in range(1, outer + 1):
        o = (mine + r) % outer
        j = o * 2 + other
        tb = fold(jnp.where(home == j // per, best, LOW), kv, jnp.maximum)
        tt = fold(jnp.where(home == j // per, total, 0.0), kv, jnp.add)
        if per > 1:
            turn = (LANES - j % per * held) % LANES
            tb, tt = pltpu.roll(tb, turn, 1), pltpu.roll(tt, turn, 1)
        mix = jnp.where(diagonal, jnp.where(lane < LANES // 2, tb, tt), 0.0)
        line = jnp.sum(mix, axis=0, keepdims=True)
        first = line.astype(jnp.bfloat16).astype(jnp.float32)
        second = (line - first).astype(jnp.bfloat16).astype(jnp.float32)
        third = line - first - second
        stats.append(jnp.where(sub == 0, first, jnp.where(sub == 1, second, third)).astype(jnp.bfloat16))
    c1.wait()
    last = []
    for r in range(1, outer + 1):
        o = (mine + r) % outer
        both = (piece(o, other) + acc_in[o].astype(jnp.float32)).astype(jnp.bfloat16)
        mail[o, :share] = both
        mail[o, share:] = stats[r - 1]
        c = remote(mail.at[o], mail_in.at[mine], as_sem.at[r - 1], ar_sem.at[mine], o * 2 + other)
        c.start()
        last.append(c)
    for o in range(outer):
        remote(mail.at[o], mail_in.at[o], as_sem.at[0], ar_sem.at[o], partner).wait_recv()
    tops = []
    for o in range(outer):
        lines = mail_in[o, share:].astype(jnp.float32)
        line = lines[0:1] + lines[1:2] + lines[2:3]
        tile = jnp.where(diagonal, line, 0.0)
        step = kv
        while step < LANES // 2:
            tile = tile + pltpu.roll(tile, step, 1)
            step *= 2
        tops.append(tile)
    best = functools.reduce(jnp.maximum, tops)
    scales = [jnp.exp2(top - best) for top in tops]
    total = sum(scale * pltpu.roll(top, LANES // 2, 1) for scale, top in zip(scales, tops))
    out = jnp.zeros((share, hd), jnp.float32)
    for o in range(outer):
        out = out + spread(scales[o] / total, LANES // 2 - kv, held) * mail_in[o, :share].astype(jnp.float32)
    out_ref[...] = out.astype(jnp.bfloat16)
    for c in sends + last:
        c.wait_send()
    for asked, _, c in direct:
        pl.when(asked)(c.wait_send)

    def handed_on():
        for c in relays:
            c.wait_send()

    pl.when(relaying)(handed_on)


def body(queries, keys, values, lengths, slot_block):
    slots, block, kv, hd = keys.shape
    share = queries.shape[0]
    n = lax.axis_size("seq")
    batch = lengths.shape[0]
    heads = n * share // batch
    group = heads // kv
    outer = n // 2
    cols = block * kv
    assert batch * kv <= LANES
    f32, bf16 = jnp.float32, jnp.bfloat16
    dma = pltpu.SemaphoreType.DMA
    vmem = pl.BlockSpec(memory_space=pltpu.VMEM)
    hbm = pl.BlockSpec(memory_space=pltpu.HBM)
    tile = (group, LANES)
    result = pl.pallas_call(
        functools.partial(kernel, n, batch, block, kv, hd ** (-0.5) * math.log2(math.e)),
        out_shape=pltpu.VMEM((share, hd), bf16),
        in_specs=[hbm] * 5,
        out_specs=vmem,
        scratch_shapes=[
            pltpu.SMEM(lengths.shape, jnp.int32),
            pltpu.SMEM(slot_block.shape, jnp.int32),
            pltpu.SMEM((batch,), jnp.int32),
            pltpu.VMEM((share, hd), bf16),
            pltpu.VMEM((n, share, hd), bf16),
            pltpu.VMEM((slots, cols, hd), bf16),
            pltpu.VMEM((slots, 2 * hd, cols // 2), bf16),
            pltpu.VMEM((slots, cols, hd), bf16),
            pltpu.VMEM((slots, group, cols), f32),
            pltpu.VMEM((slots + 1, heads, hd), f32),
            pltpu.VMEM((slots, *tile), f32),
            pltpu.VMEM((slots, *tile), f32),
            pltpu.VMEM(tile, f32),
            pltpu.VMEM(tile, f32),
            pltpu.VMEM(tile, f32),
            pltpu.VMEM(tile, f32),
            pltpu.VMEM((outer, share, hd), bf16),
            pltpu.VMEM((outer, share, hd), bf16),
            pltpu.VMEM((outer, share + group, hd), bf16),
            pltpu.VMEM((outer, share + group, hd), bf16),
            dma((slots,)), dma((slots,)), dma, dma((3,)),
            dma((outer,)), dma((n,)), dma((outer,)), dma((outer,)), pltpu.SemaphoreType.REGULAR, dma((6,)),
            dma((outer,)), dma((outer,)),
        ],
        compiler_params=pltpu.CompilerParams(
            collective_id=0, has_side_effects=True, vmem_limit_bytes=67043328 - max(share * hd * 2, 2**14)
        ),
        name="decode",
    )(
        lengths,
        slot_block,
        queries.reshape(share, hd),
        keys.reshape(slots, cols, hd),
        values.reshape(slots, cols, hd),
    )
    return result.reshape(share, 1, hd)


def solution(mesh):
    placed = (
        P(("grp", "seq"), "head", None),
        P(("grp", "seq"), None, "head", None),
        P(("grp", "seq"), None, "head", None),
        P("grp"),
        P(("grp", "seq")),
    )
    return jax.shard_map(
        body, mesh=mesh, in_specs=placed, out_specs=P(("grp", "seq"), "head", None), check_vma=False
    )
```

```python
import functools
import math
import jax
import jax.numpy as jnp
from jax import lax
from jax.experimental import pallas as pl
from jax.experimental.pallas import tpu as pltpu
from jax.sharding import PartitionSpec as P

LANES = 128
MESH_ID = pl.DeviceIdType.MESH
LOW = -1e30
DEAD = -3e38
PLANE = 2
LATE = 4


def fold(tile, step, op):
    shift = LANES // 2
    while shift >= step:
        tile = op(tile, pltpu.roll(tile, shift, 1))
        shift //= 2
    return tile


def spread(tile, start, heads):
    group = tile.shape[0]
    return jnp.concatenate(
        [jnp.broadcast_to(tile[:, start + h : start + h + 1], (group, LANES)) for h in range(heads)],
        axis=0,
    )


def kernel(
    n, batch, block, kv, factor,
    lengths_hbm, block_hbm, q_hbm, k_hbm, v_hbm, out_ref,
    lengths, slot_block, final, q_ref, q_all, k_buf, k_turn, v_buf, scores, sums, peaks, totals,
    best_own, best_in, tot_own, tot_in, acc_send, acc_in, mail, mail_in,
    k_sem, v_sem, own_sem, in_sem, qs_sem, qr_sem, fs_sem, relay_sem, ready, swap_sem, as_sem, ar_sem,
):
    slots, cols, hd = k_buf.shape
    share = q_ref.shape[0]
    outer = n // 2
    per = n // batch
    blocks = slots * n // batch
    heads = per * share
    group = heads // kv
    held = share // group
    half = cols // 2
    lead = slots - slots // LATE
    me = lax.axis_index("seq")
    mine, inner = me // 2, me % 2
    other = 1 - inner
    partner = me + 1 - 2 * inner

    def k_copy(s):
        return pltpu.make_async_copy(k_hbm.at[s], k_buf.at[s], k_sem.at[s])

    def v_copy(s):
        return pltpu.make_async_copy(v_hbm.at[s], v_buf.at[s], v_sem.at[s])

    def remote(src, dst, ssem, rsem, dev):
        return pltpu.make_async_remote_copy(
            src_ref=src, dst_ref=dst, send_sem=ssem, recv_sem=rsem,
            device_id={"seq": dev}, device_id_type=MESH_ID,
        )

    q_in = pltpu.make_async_copy(q_hbm, q_ref, in_sem.at[0])
    q_in.start()
    edge = outer - PLANE
    late = mine >= edge
    front, relaying = mine < PLANE, jnp.logical_and(mine >= PLANE, mine < 2 * PLANE)
    peers = [(mine + jnp.where(relaying, outer - r, r)) % outer for r in range(1, outer)]
    barrier = pltpu.get_barrier_semaphore()

    def greet(o):
        pl.semaphore_signal(barrier, inc=1, device_id={"seq": o * 2 + other}, device_id_type=MESH_ID)

    for o in peers:
        asks = jnp.where(late, o >= edge, front | (o >= PLANE) | (o + PLANE == mine))
        pl.when(asks)(functools.partial(greet, o))
    pl.semaphore_signal(barrier, inc=1, device_id={"seq": partner}, device_id_type=MESH_ID)
    len_in = pltpu.make_async_copy(lengths_hbm, lengths, in_sem.at[1])
    block_in = pltpu.make_async_copy(block_hbm, slot_block, in_sem.at[2])
    len_in.start()
    block_in.start()
    own = pltpu.make_async_copy(q_hbm, q_all.at[me], own_sem)
    own.start()
    for s in range(slots):
        k_copy(s).start()
    for s in range(slots):
        v_copy(s).start(priority=1)
    q_in.wait()
    chunk = min(half, 256)

    def turn_keys():
        def one(s, carry):
            k_copy(s).wait()
            for c in range(0, half, chunk):
                k_turn[s, :hd, c : c + chunk] = k_buf[s, c : c + chunk, :].T
                k_turn[s, hd:, c : c + chunk] = k_buf[s, half + c : half + c + chunk, :].T
            return carry
        lax.fori_loop(0, slots, one, 0)

    pl.semaphore_wait(barrier, jnp.where(front, PLANE + 1, jnp.where(late, outer, edge)))

    def announce():
        for o in range(PLANE, edge):
            pl.semaphore_signal(ready, inc=1, device_id={"seq": o * 2 + other}, device_id_type=MESH_ID)

    pl.when(late)(announce)
    direct = []
    for r, o in enumerate(peers):
        c = remote(q_ref, q_all.at[me], qs_sem.at[r], qr_sem.at[me], o * 2 + other)
        asked = jnp.logical_not(front) | (o < PLANE) | (o == mine + PLANE)
        direct.append((asked, late | (o < edge), c))
    for asked, soon, c in direct:
        pl.when(asked & soon)(c.start)
    sends = [remote(q_ref, q_all.at[me], qs_sem.at[outer - 1], qr_sem.at[me], partner)]
    sends[0].start()
    origin = (mine + outer - PLANE) % outer * 2 + other
    targets = [outer - 1 - t for t in range(PLANE)]
    targets += [PLANE + (mine + t) % PLANE for t in range(1, PLANE)]
    targets += [edge - 1 - t for t in range(edge - 2 * PLANE)]
    relays = [
        remote(q_all.at[origin], q_all.at[origin], relay_sem.at[t], qr_sem.at[origin], o * 2 + other)
        for t, o in enumerate(targets)
    ]

    def receive_first():
        remote(q_ref, q_all.at[origin], qs_sem.at[0], qr_sem.at[origin], partner).wait_recv()
        for c in relays[PLANE : 2 * PLANE - 1]:
            c.start()

    def hand_on():
        for c in relays[:PLANE]:
            c.start()

    def hand_back():
        for c in relays[2 * PLANE - 1 :]:
            c.start()

    def side(o):
        return jnp.where(jnp.logical_not(front) & (o < PLANE) & (o + PLANE != mine), inner, other)

    pl.when(relaying)(receive_first)

    def wait_late():
        pl.semaphore_wait(ready, PLANE)

    pl.when(relaying)(hand_back)
    pl.when(jnp.logical_not(front | late))(wait_late)
    pl.when(relaying)(hand_on)
    for asked, soon, c in direct:
        pl.when(asked & jnp.logical_not(soon))(c.start)
    sums[...] = jnp.zeros_like(sums)
    len_in.wait()
    block_in.wait()
    seqs = [slot_block[s] // blocks for s in range(slots)]
    before = []
    for s in range(slots):
        prev = slots
        for t in range(s):
            prev = jnp.where(seqs[t] == seqs[s], t, prev)
        before.append(prev)
    for b in range(batch):
        last = slots
        for s in range(slots):
            last = jnp.where(seqs[s] == b, s, last)
        final[b] = last
    turn_keys()
    for r in range(1, outer):
        o = (mine + outer - r) % outer
        src = o * 2 + side(o)
        arrival = remote(q_ref, q_all.at[src], qs_sem.at[0], qr_sem.at[src], partner)
        if r == PLANE:
            pl.when(jnp.logical_not(relaying))(arrival.wait_recv)
        else:
            arrival.wait_recv()
        c = remote(q_all.at[src], q_all.at[src], fs_sem.at[r - 1], qr_sem.at[src], partner)
        c.start()
        sends.append(c)
    own.wait()
    remote(q_ref, q_all.at[partner], qs_sem.at[0], qr_sem.at[partner], partner).wait_recv()
    for r in range(1, outer):
        o = (mine + outer - r) % outer
        src = o * 2 + 1 - side(o)
        remote(q_ref, q_all.at[src], qs_sem.at[0], qr_sem.at[src], partner).wait_recv()

    lane = lax.broadcasted_iota(jnp.int32, (group, LANES), 1)
    home = lane // kv
    wide = lax.broadcasted_iota(jnp.int32, (group, chunk), 1)
    picks = [wide % kv == h for h in range(kv)]

    def score(s):
        code = slot_block[s]
        seq, blk = code // blocks, code % blocks
        limit = (lengths[seq] - blk * block) * kv
        q = q_all[pl.ds(seq * per, per)]
        if per > 1:
            q = q.astype(jnp.float32).reshape(heads, hd).astype(jnp.bfloat16)
        else:
            q = q.reshape(heads, hd)
        blank = jnp.zeros_like(q)
        both = jnp.concatenate(
            [jnp.concatenate([q, blank], axis=0), jnp.concatenate([blank, q], axis=0)], axis=1
        )
        top = jnp.full((group, LANES), LOW, jnp.float32)
        for c in range(0, half, chunk):
            full = jnp.dot(both, k_turn[s, :, c : c + chunk], preferred_element_type=jnp.float32)
            for x, at in ((0, c), (heads, half + c)):
                packed = full[x : x + group]
                for h in range(1, kv):
                    packed = jnp.where(picks[h], full[x + h * group : x + (h + 1) * group], packed)
                packed = jnp.where(wide < limit - at, packed * factor, DEAD)
                scores[s, :, at : at + chunk] = packed
                for l in range(0, chunk, LANES):
                    top = jnp.maximum(top, packed[:, l : l + LANES])
        peaks[s] = fold(top, kv, jnp.maximum)

    def weigh(s):
        top = jnp.concatenate([peaks[s]] * (chunk // LANES), axis=1)
        total = jnp.zeros((group, LANES), jnp.float32)
        out = jnp.zeros((2 * heads, 2 * hd), jnp.float32)
        for c in range(0, half, chunk):
            rows = []
            for at in (c, half + c):
                weight = jnp.exp2(scores[s, :, at : at + chunk] - top).astype(jnp.bfloat16)
                weight = weight.astype(jnp.float32)
                for l in range(0, chunk, LANES):
                    total = total + weight[:, l : l + LANES]
                rows += [jnp.where(picks[h], weight, 0.0) for h in range(kv)]
            vals = jnp.concatenate(
                [v_buf[s, c : c + chunk, :], v_buf[s, half + c : half + c + chunk, :]], axis=1
            )
            out = out + jnp.dot(
                jnp.concatenate(rows, axis=0).astype(jnp.bfloat16), vals,
                preferred_element_type=jnp.float32,
            )
        sums[s] = out[:heads, :hd] + out[heads:, hd:]
        totals[s] = fold(total, kv, jnp.add)

    def loop(step, start, end):
        def one(s, carry):
            step(s)
            return carry
        lax.fori_loop(start, end, one, 0, unroll=True)

    for s in range(slots):
        v_copy(s).wait()
    loop(score, 0, slots)
    best = jnp.full((group, LANES), LOW, jnp.float32)
    for s in range(slots):
        best = jnp.maximum(best, jnp.where(home == seqs[s], peaks[s], LOW))
    best_own[...] = best
    swap = remote(best_own, best_in, swap_sem.at[0], swap_sem.at[1], partner)
    weigh(0)
    swap.start()
    loop(weigh, 1, lead)
    swap.wait()
    best = jnp.maximum(best_own[...], best_in[...])

    def gather(s, total):
        ours = fold(jnp.where(home == seqs[s], best, LOW), kv, jnp.maximum)
        scale = jnp.exp2(peaks[s] - ours)
        sums[s] = sums[s] * spread(scale, 0, kv) + sums[before[s]]
        return total + jnp.where(home == seqs[s], totals[s] * scale, 0.0)

    total = jnp.zeros((group, LANES), jnp.float32)
    done = 0
    for s in range(lead, slots):
        weigh(s)
        upto = lead * (s + 1 - lead) // (slots - lead)
        for t in range(done, upto):
            total = gather(t, total)
        done = upto
    for t in range(done, slots):
        total = gather(t, total)

    def piece(o, core):
        j = o * 2 + core
        if per == 1:
            return sums[final[j]]
        return sums[final[j // per], pl.ds(pl.multiple_of(j % per * share, share), share), :]

    sub = lax.broadcasted_iota(jnp.int32, (group, LANES), 0)
    diagonal = lane % (LANES // 2) // kv == sub
    tot_own[...] = total
    c2 = remote(tot_own, tot_in, swap_sem.at[2], swap_sem.at[3], partner)
    c2.start()
    shares = []
    for h in range(2):
        at = pl.ds(h * (outer // 2), outer // 2)
        for r in range(h * (outer // 2), (h + 1) * (outer // 2)):
            acc_send[r] = piece((mine + r + 1) % outer, inner).astype(jnp.bfloat16)
        c = remote(acc_send.at[at], acc_in.at[at], swap_sem.at[4 + h], swap_sem.at[6 + h], partner)
        c.start()
        shares.append(c)
    c2.wait()
    total = tot_own[...] + tot_in[...]
    stats = []
    for r in range(1, outer + 1):
        o = (mine + r) % outer
        j = o * 2 + other
        tb = fold(jnp.where(home == j // per, best, LOW), kv, jnp.maximum)
        tt = fold(jnp.where(home == j // per, total, 0.0), kv, jnp.add)
        if per > 1:
            turn = (LANES - j % per * held) % LANES
            tb, tt = pltpu.roll(tb, turn, 1), pltpu.roll(tt, turn, 1)
        mix = jnp.where(diagonal, jnp.where(lane < LANES // 2, tb, tt), 0.0)
        line = jnp.sum(mix, axis=0, keepdims=True)
        first = line.astype(jnp.bfloat16).astype(jnp.float32)
        second = (line - first).astype(jnp.bfloat16).astype(jnp.float32)
        third = line - first - second
        stats.append(jnp.where(sub == 0, first, jnp.where(sub == 1, second, third)).astype(jnp.bfloat16))
    last = []
    for r in range(1, outer + 1):
        o = (mine + r) % outer
        if (r - 1) % (outer // 2) == 0:
            shares[(r - 1) // (outer // 2)].wait()
        both = (piece(o, other) + acc_in[r - 1].astype(jnp.float32)).astype(jnp.bfloat16)
        mail[o, :share] = both
        mail[o, share:] = stats[r - 1]
        c = remote(mail.at[o], mail_in.at[mine], as_sem.at[r - 1], ar_sem.at[mine], o * 2 + other)
        c.start()
        last.append(c)
    for o in range(outer):
        remote(mail.at[o], mail_in.at[o], as_sem.at[0], ar_sem.at[o], partner).wait_recv()
    tops = []
    for o in range(outer):
        lines = mail_in[o, share:].astype(jnp.float32)
        line = lines[0:1] + lines[1:2] + lines[2:3]
        tile = jnp.where(diagonal, line, 0.0)
        step = kv
        while step < LANES // 2:
            tile = tile + pltpu.roll(tile, step, 1)
            step *= 2
        tops.append(tile)
    best = functools.reduce(jnp.maximum, tops)
    scales = [jnp.exp2(top - best) for top in tops]
    total = sum(scale * pltpu.roll(top, LANES // 2, 1) for scale, top in zip(scales, tops))
    out = jnp.zeros((share, hd), jnp.float32)
    for o in range(outer):
        out = out + spread(scales[o] / total, LANES // 2 - kv, held) * mail_in[o, :share].astype(jnp.float32)
    out_ref[...] = out.astype(jnp.bfloat16)
    for c in sends + last:
        c.wait_send()
    for asked, _, c in direct:
        pl.when(asked)(c.wait_send)

    def handed_on():
        for c in relays:
            c.wait_send()

    pl.when(relaying)(handed_on)


def body(queries, keys, values, lengths, slot_block):
    slots, block, kv, hd = keys.shape
    share = queries.shape[0]
    n = lax.axis_size("seq")
    batch = lengths.shape[0]
    heads = n * share // batch
    group = heads // kv
    outer = n // 2
    cols = block * kv
    assert batch * kv <= LANES
    f32, bf16 = jnp.float32, jnp.bfloat16
    dma = pltpu.SemaphoreType.DMA
    vmem = pl.BlockSpec(memory_space=pltpu.VMEM)
    hbm = pl.BlockSpec(memory_space=pltpu.HBM)
    tile = (group, LANES)
    result = pl.pallas_call(
        functools.partial(kernel, n, batch, block, kv, hd ** (-0.5) * math.log2(math.e)),
        out_shape=pltpu.VMEM((share, hd), bf16),
        in_specs=[hbm] * 5,
        out_specs=vmem,
        scratch_shapes=[
            pltpu.SMEM(lengths.shape, jnp.int32),
            pltpu.SMEM(slot_block.shape, jnp.int32),
            pltpu.SMEM((batch,), jnp.int32),
            pltpu.VMEM((share, hd), bf16),
            pltpu.VMEM((n, share, hd), bf16),
            pltpu.VMEM((slots, cols, hd), bf16),
            pltpu.VMEM((slots, 2 * hd, cols // 2), bf16),
            pltpu.VMEM((slots, cols, hd), bf16),
            pltpu.VMEM((slots, group, cols), f32),
            pltpu.VMEM((slots + 1, heads, hd), f32),
            pltpu.VMEM((slots, *tile), f32),
            pltpu.VMEM((slots, *tile), f32),
            pltpu.VMEM(tile, f32),
            pltpu.VMEM(tile, f32),
            pltpu.VMEM(tile, f32),
            pltpu.VMEM(tile, f32),
            pltpu.VMEM((outer, share, hd), bf16),
            pltpu.VMEM((outer, share, hd), bf16),
            pltpu.VMEM((outer, share + group, hd), bf16),
            pltpu.VMEM((outer, share + group, hd), bf16),
            dma((slots,)), dma((slots,)), dma, dma((3,)),
            dma((outer,)), dma((n,)), dma((outer,)), dma((outer,)), pltpu.SemaphoreType.REGULAR, dma((8,)),
            dma((outer,)), dma((outer,)),
        ],
        compiler_params=pltpu.CompilerParams(
            collective_id=0, has_side_effects=True, vmem_limit_bytes=67043328 - max(share * hd * 2, 2**14)
        ),
        name="decode",
    )(
        lengths,
        slot_block,
        queries.reshape(share, hd),
        keys.reshape(slots, cols, hd),
        values.reshape(slots, cols, hd),
    )
    return result.reshape(share, 1, hd)


def solution(mesh):
    placed = (
        P(("grp", "seq"), "head", None),
        P(("grp", "seq"), None, "head", None),
        P(("grp", "seq"), None, "head", None),
        P("grp"),
        P(("grp", "seq")),
    )
    return jax.shard_map(
        body, mesh=mesh, in_specs=placed, out_specs=P(("grp", "seq"), "head", None), check_vma=False
    )
```

```python
import functools
import math
import jax
import jax.numpy as jnp
from jax import lax
from jax.experimental import pallas as pl
from jax.experimental.pallas import tpu as pltpu
from jax.sharding import PartitionSpec as P

LANES = 128
MESH_ID = pl.DeviceIdType.MESH
LOW = -1e30
DEAD = -3e38
PLANE = 2
LATE = 8


def fold(tile, step, op):
    shift = LANES // 2
    while shift >= step:
        tile = op(tile, pltpu.roll(tile, shift, 1))
        shift //= 2
    return tile


def spread(tile, start, heads):
    group = tile.shape[0]
    return jnp.concatenate(
        [jnp.broadcast_to(tile[:, start + h : start + h + 1], (group, LANES)) for h in range(heads)],
        axis=0,
    )


def kernel(
    n, batch, block, kv, factor,
    lengths_hbm, block_hbm, q_hbm, k_hbm, v_hbm, out_ref,
    lengths, slot_block, final, q_ref, q_all, k_buf, k_turn, v_buf, scores, sums, peaks, totals,
    best_own, best_in, tot_own, tot_in, acc_send, acc_in, mail, mail_in,
    k_sem, v_sem, own_sem, in_sem, qs_sem, qr_sem, fs_sem, relay_sem, ready, swap_sem, as_sem, ar_sem,
):
    slots, cols, hd = k_buf.shape
    share = q_ref.shape[0]
    outer = n // 2
    per = n // batch
    blocks = slots * n // batch
    heads = per * share
    group = heads // kv
    held = share // group
    half = cols // 2
    lead = slots - slots // LATE
    me = lax.axis_index("seq")
    mine, inner = me // 2, me % 2
    other = 1 - inner
    partner = me + 1 - 2 * inner

    def k_copy(s):
        return pltpu.make_async_copy(k_hbm.at[s], k_buf.at[s], k_sem.at[s])

    def v_copy(s):
        return pltpu.make_async_copy(v_hbm.at[s], v_buf.at[s], v_sem.at[s])

    def remote(src, dst, ssem, rsem, dev):
        return pltpu.make_async_remote_copy(
            src_ref=src, dst_ref=dst, send_sem=ssem, recv_sem=rsem,
            device_id={"seq": dev}, device_id_type=MESH_ID,
        )

    q_in = pltpu.make_async_copy(q_hbm, q_ref, in_sem.at[0])
    q_in.start()
    edge = outer - PLANE
    late = mine >= edge
    front, relaying = mine < PLANE, jnp.logical_and(mine >= PLANE, mine < 2 * PLANE)
    peers = [(mine + jnp.where(relaying, outer - r, r)) % outer for r in range(1, outer)]
    barrier = pltpu.get_barrier_semaphore()

    def greet(o):
        pl.semaphore_signal(barrier, inc=1, device_id={"seq": o * 2 + other}, device_id_type=MESH_ID)

    for o in peers:
        asks = jnp.where(late, o >= edge, front | (o >= PLANE) | (o + PLANE == mine))
        pl.when(asks)(functools.partial(greet, o))
    pl.semaphore_signal(barrier, inc=1, device_id={"seq": partner}, device_id_type=MESH_ID)
    len_in = pltpu.make_async_copy(lengths_hbm, lengths, in_sem.at[1])
    block_in = pltpu.make_async_copy(block_hbm, slot_block, in_sem.at[2])
    len_in.start()
    block_in.start()
    own = pltpu.make_async_copy(q_hbm, q_all.at[me], own_sem)
    own.start()
    for s in range(slots):
        k_copy(s).start()
    for s in range(slots):
        v_copy(s).start(priority=1)
    q_in.wait()
    chunk = min(half, 256)

    def turn_keys():
        def one(s, carry):
            k_copy(s).wait()
            for c in range(0, half, chunk):
                k_turn[s, :hd, c : c + chunk] = k_buf[s, c : c + chunk, :].T
                k_turn[s, hd:, c : c + chunk] = k_buf[s, half + c : half + c + chunk, :].T
            return carry
        lax.fori_loop(0, slots, one, 0)

    pl.semaphore_wait(barrier, jnp.where(front, PLANE + 1, jnp.where(late, outer, edge)))

    def announce():
        for o in range(PLANE, edge):
            pl.semaphore_signal(ready, inc=1, device_id={"seq": o * 2 + other}, device_id_type=MESH_ID)

    pl.when(late)(announce)
    direct = []
    for r, o in enumerate(peers):
        c = remote(q_ref, q_all.at[me], qs_sem.at[r], qr_sem.at[me], o * 2 + other)
        asked = jnp.logical_not(front) | (o < PLANE) | (o == mine + PLANE)
        direct.append((asked, late | (o < edge), c))
    for asked, soon, c in direct:
        pl.when(asked & soon)(c.start)
    sends = [remote(q_ref, q_all.at[me], qs_sem.at[outer - 1], qr_sem.at[me], partner)]
    sends[0].start()
    origin = (mine + outer - PLANE) % outer * 2 + other
    targets = [outer - 1 - t for t in range(PLANE)]
    targets += [PLANE + (mine + t) % PLANE for t in range(1, PLANE)]
    targets += [edge - 1 - t for t in range(edge - 2 * PLANE)]
    relays = [
        remote(q_all.at[origin], q_all.at[origin], relay_sem.at[t], qr_sem.at[origin], o * 2 + other)
        for t, o in enumerate(targets)
    ]

    def receive_first():
        remote(q_ref, q_all.at[origin], qs_sem.at[0], qr_sem.at[origin], partner).wait_recv()
        for c in relays[PLANE : 2 * PLANE - 1]:
            c.start()

    def hand_on():
        for c in relays[:PLANE]:
            c.start()

    def hand_back():
        for c in relays[2 * PLANE - 1 :]:
            c.start()

    def side(o):
        return jnp.where(jnp.logical_not(front) & (o < PLANE) & (o + PLANE != mine), inner, other)

    pl.when(relaying)(receive_first)

    def wait_late():
        pl.semaphore_wait(ready, PLANE)

    pl.when(relaying)(hand_back)
    pl.when(jnp.logical_not(front | late))(wait_late)
    pl.when(relaying)(hand_on)
    for asked, soon, c in direct:
        pl.when(asked & jnp.logical_not(soon))(c.start)
    sums[...] = jnp.zeros_like(sums)
    len_in.wait()
    block_in.wait()
    seqs = [slot_block[s] // blocks for s in range(slots)]
    before = []
    for s in range(slots):
        prev = slots
        for t in range(s):
            prev = jnp.where(seqs[t] == seqs[s], t, prev)
        before.append(prev)
    for b in range(batch):
        last = slots
        for s in range(slots):
            last = jnp.where(seqs[s] == b, s, last)
        final[b] = last
    turn_keys()
    for r in range(1, outer):
        o = (mine + outer - r) % outer
        src = o * 2 + side(o)
        arrival = remote(q_ref, q_all.at[src], qs_sem.at[0], qr_sem.at[src], partner)
        if r == PLANE:
            pl.when(jnp.logical_not(relaying))(arrival.wait_recv)
        else:
            arrival.wait_recv()
        c = remote(q_all.at[src], q_all.at[src], fs_sem.at[r - 1], qr_sem.at[src], partner)
        c.start()
        sends.append(c)
    own.wait()
    remote(q_ref, q_all.at[partner], qs_sem.at[0], qr_sem.at[partner], partner).wait_recv()
    for r in range(1, outer):
        o = (mine + outer - r) % outer
        src = o * 2 + 1 - side(o)
        remote(q_ref, q_all.at[src], qs_sem.at[0], qr_sem.at[src], partner).wait_recv()

    lane = lax.broadcasted_iota(jnp.int32, (group, LANES), 1)
    home = lane // kv
    wide = lax.broadcasted_iota(jnp.int32, (group, chunk), 1)
    picks = [wide % kv == h for h in range(kv)]

    def score(s):
        code = slot_block[s]
        seq, blk = code // blocks, code % blocks
        limit = (lengths[seq] - blk * block) * kv
        q = q_all[pl.ds(seq * per, per)]
        if per > 1:
            q = q.astype(jnp.float32).reshape(heads, hd).astype(jnp.bfloat16)
        else:
            q = q.reshape(heads, hd)
        blank = jnp.zeros_like(q)
        both = jnp.concatenate(
            [jnp.concatenate([q, blank], axis=0), jnp.concatenate([blank, q], axis=0)], axis=1
        )
        top = jnp.full((group, LANES), LOW, jnp.float32)
        for c in range(0, half, chunk):
            full = jnp.dot(both, k_turn[s, :, c : c + chunk], preferred_element_type=jnp.float32)
            for x, at in ((0, c), (heads, half + c)):
                packed = full[x : x + group]
                for h in range(1, kv):
                    packed = jnp.where(picks[h], full[x + h * group : x + (h + 1) * group], packed)
                packed = jnp.where(wide < limit - at, packed * factor, DEAD)
                scores[s, :, at : at + chunk] = packed
                for l in range(0, chunk, LANES):
                    top = jnp.maximum(top, packed[:, l : l + LANES])
        peaks[s] = fold(top, kv, jnp.maximum)

    def weigh(s):
        top = jnp.concatenate([peaks[s]] * (chunk // LANES), axis=1)
        total = jnp.zeros((group, LANES), jnp.float32)
        out = jnp.zeros((2 * heads, 2 * hd), jnp.float32)
        for c in range(0, half, chunk):
            rows = []
            for at in (c, half + c):
                weight = jnp.exp2(scores[s, :, at : at + chunk] - top).astype(jnp.bfloat16)
                weight = weight.astype(jnp.float32)
                for l in range(0, chunk, LANES):
                    total = total + weight[:, l : l + LANES]
                rows += [jnp.where(picks[h], weight, 0.0) for h in range(kv)]
            vals = jnp.concatenate(
                [v_buf[s, c : c + chunk, :], v_buf[s, half + c : half + c + chunk, :]], axis=1
            )
            out = out + jnp.dot(
                jnp.concatenate(rows, axis=0).astype(jnp.bfloat16), vals,
                preferred_element_type=jnp.float32,
            )
        sums[s] = out[:heads, :hd] + out[heads:, hd:]
        totals[s] = fold(total, kv, jnp.add)

    def loop(step, start, end):
        def one(s, carry):
            step(s)
            return carry
        lax.fori_loop(start, end, one, 0, unroll=True)

    for s in range(slots):
        v_copy(s).wait()
    loop(score, 0, slots)
    best = jnp.full((group, LANES), LOW, jnp.float32)
    for s in range(slots):
        best = jnp.maximum(best, jnp.where(home == seqs[s], peaks[s], LOW))
    best_own[...] = best
    swap = remote(best_own, best_in, swap_sem.at[0], swap_sem.at[1], partner)
    weigh(0)
    swap.start()
    loop(weigh, 1, lead)
    swap.wait()
    best = jnp.maximum(best_own[...], best_in[...])

    def gather(s, total):
        ours = fold(jnp.where(home == seqs[s], best, LOW), kv, jnp.maximum)
        scale = jnp.exp2(peaks[s] - ours)
        sums[s] = sums[s] * spread(scale, 0, kv) + sums[before[s]]
        return total + jnp.where(home == seqs[s], totals[s] * scale, 0.0)

    total = jnp.zeros((group, LANES), jnp.float32)
    done = 0
    for s in range(lead, slots):
        weigh(s)
        upto = lead * (s + 1 - lead) // (slots - lead)
        for t in range(done, upto):
            total = gather(t, total)
        done = upto
    for t in range(done, slots):
        total = gather(t, total)

    def piece(o, core):
        j = o * 2 + core
        if per == 1:
            return sums[final[j]]
        return sums[final[j // per], pl.ds(pl.multiple_of(j % per * share, share), share), :]

    sub = lax.broadcasted_iota(jnp.int32, (group, LANES), 0)
    diagonal = lane % (LANES // 2) // kv == sub
    tot_own[...] = total
    c2 = remote(tot_own, tot_in, swap_sem.at[2], swap_sem.at[3], partner)
    c2.start()
    shares = []
    for h in range(2):
        at = pl.ds(h * (outer // 2), outer // 2)
        for r in range(h * (outer // 2), (h + 1) * (outer // 2)):
            acc_send[r] = piece((mine + r + 1) % outer, inner).astype(jnp.bfloat16)
        c = remote(acc_send.at[at], acc_in.at[at], swap_sem.at[4 + h], swap_sem.at[6 + h], partner)
        c.start()
        shares.append(c)
    c2.wait()
    total = tot_own[...] + tot_in[...]
    stats = []
    for r in range(1, outer + 1):
        o = (mine + r) % outer
        j = o * 2 + other
        tb = fold(jnp.where(home == j // per, best, LOW), kv, jnp.maximum)
        tt = fold(jnp.where(home == j // per, total, 0.0), kv, jnp.add)
        if per > 1:
            turn = (LANES - j % per * held) % LANES
            tb, tt = pltpu.roll(tb, turn, 1), pltpu.roll(tt, turn, 1)
        mix = jnp.where(diagonal, jnp.where(lane < LANES // 2, tb, tt), 0.0)
        line = jnp.sum(mix, axis=0, keepdims=True)
        first = line.astype(jnp.bfloat16).astype(jnp.float32)
        second = (line - first).astype(jnp.bfloat16).astype(jnp.float32)
        third = line - first - second
        stats.append(jnp.where(sub == 0, first, jnp.where(sub == 1, second, third)).astype(jnp.bfloat16))
    last = []
    for r in range(1, outer + 1):
        o = (mine + r) % outer
        if (r - 1) % (outer // 2) == 0:
            shares[(r - 1) // (outer // 2)].wait()
        both = (piece(o, other) + acc_in[r - 1].astype(jnp.float32)).astype(jnp.bfloat16)
        mail[o, :share] = both
        mail[o, share:] = stats[r - 1]
        c = remote(mail.at[o], mail_in.at[mine], as_sem.at[r - 1], ar_sem.at[mine], o * 2 + other)
        c.start()
        last.append(c)
    for o in range(outer):
        remote(mail.at[o], mail_in.at[o], as_sem.at[0], ar_sem.at[o], partner).wait_recv()
    tops = []
    for o in range(outer):
        lines = mail_in[o, share:].astype(jnp.float32)
        line = lines[0:1] + lines[1:2] + lines[2:3]
        tile = jnp.where(diagonal, line, 0.0)
        step = kv
        while step < LANES // 2:
            tile = tile + pltpu.roll(tile, step, 1)
            step *= 2
        tops.append(tile)
    best = functools.reduce(jnp.maximum, tops)
    scales = [jnp.exp2(top - best) for top in tops]
    total = sum(scale * pltpu.roll(top, LANES // 2, 1) for scale, top in zip(scales, tops))
    out = jnp.zeros((share, hd), jnp.float32)
    for o in range(outer):
        out = out + spread(scales[o] / total, LANES // 2 - kv, held) * mail_in[o, :share].astype(jnp.float32)
    out_ref[...] = out.astype(jnp.bfloat16)
    for c in sends + last:
        c.wait_send()
    for asked, _, c in direct:
        pl.when(asked)(c.wait_send)

    def handed_on():
        for c in relays:
            c.wait_send()

    pl.when(relaying)(handed_on)


def body(queries, keys, values, lengths, slot_block):
    slots, block, kv, hd = keys.shape
    share = queries.shape[0]
    n = lax.axis_size("seq")
    batch = lengths.shape[0]
    heads = n * share // batch
    group = heads // kv
    outer = n // 2
    cols = block * kv
    assert batch * kv <= LANES
    f32, bf16 = jnp.float32, jnp.bfloat16
    dma = pltpu.SemaphoreType.DMA
    vmem = pl.BlockSpec(memory_space=pltpu.VMEM)
    hbm = pl.BlockSpec(memory_space=pltpu.HBM)
    tile = (group, LANES)
    result = pl.pallas_call(
        functools.partial(kernel, n, batch, block, kv, hd ** (-0.5) * math.log2(math.e)),
        out_shape=pltpu.VMEM((share, hd), bf16),
        in_specs=[hbm] * 5,
        out_specs=vmem,
        scratch_shapes=[
            pltpu.SMEM(lengths.shape, jnp.int32),
            pltpu.SMEM(slot_block.shape, jnp.int32),
            pltpu.SMEM((batch,), jnp.int32),
            pltpu.VMEM((share, hd), bf16),
            pltpu.VMEM((n, share, hd), bf16),
            pltpu.VMEM((slots, cols, hd), bf16),
            pltpu.VMEM((slots, 2 * hd, cols // 2), bf16),
            pltpu.VMEM((slots, cols, hd), bf16),
            pltpu.VMEM((slots, group, cols), f32),
            pltpu.VMEM((slots + 1, heads, hd), f32),
            pltpu.VMEM((slots, *tile), f32),
            pltpu.VMEM((slots, *tile), f32),
            pltpu.VMEM(tile, f32),
            pltpu.VMEM(tile, f32),
            pltpu.VMEM(tile, f32),
            pltpu.VMEM(tile, f32),
            pltpu.VMEM((outer, share, hd), bf16),
            pltpu.VMEM((outer, share, hd), bf16),
            pltpu.VMEM((outer, share + group, hd), bf16),
            pltpu.VMEM((outer, share + group, hd), bf16),
            dma((slots,)), dma((slots,)), dma, dma((3,)),
            dma((outer,)), dma((n,)), dma((outer,)), dma((outer,)), pltpu.SemaphoreType.REGULAR, dma((8,)),
            dma((outer,)), dma((outer,)),
        ],
        compiler_params=pltpu.CompilerParams(
            collective_id=0, has_side_effects=True, vmem_limit_bytes=67043328 - max(share * hd * 2, 2**14)
        ),
        name="decode",
    )(
        lengths,
        slot_block,
        queries.reshape(share, hd),
        keys.reshape(slots, cols, hd),
        values.reshape(slots, cols, hd),
    )
    return result.reshape(share, 1, hd)


def solution(mesh):
    placed = (
        P(("grp", "seq"), "head", None),
        P(("grp", "seq"), None, "head", None),
        P(("grp", "seq"), None, "head", None),
        P("grp"),
        P(("grp", "seq")),
    )
    return jax.shard_map(
        body, mesh=mesh, in_specs=placed, out_specs=P(("grp", "seq"), "head", None), check_vma=False
    )
```
